512 devices in a mesh: gx: 16 (over x, z_hi), gy: 32 (over z_lo, y, core).
Axes of the slice: x: 4, y: 4, z: 16 (z_hi: 4, z_lo: 4; z = z_hi * 4 + z_lo), core: 2. Of those that a mesh axis runs over, the one named last changes fastest.
Arguments:
- fields: float32 [3, 512, 4096], P(None, 'gx', 'gy'), may hold values from -10 to 10
- lift_weight: float32 [12, 64], replicated, may hold values from -1.75 to 1.75
- lift_bias: float32 [64], replicated, may hold values from -3 to 3
- spectral_weight: float32 [2, 8, 8, 64, 64], replicated, may hold values from -4 to 4
- bypass_weight: float32 [64, 64], replicated, may hold values from -0.75 to 0.75
- layer_bias: float32 [64], replicated, may hold values from -3 to 3
- mlp_in_weight: float32 [64, 128], replicated, may hold values from -0.75 to 0.75
- mlp_in_bias: float32 [128], replicated, may hold values from -3 to 3
- mlp_out_weight: float32 [128, 64], replicated, may hold values from -0.5 to 0.5
- mlp_out_bias: float32 [64], replicated, may hold values from -3 to 3
- project_weight: float32 [64, 3], replicated, may hold values from -0.75 to 0.75
- project_bias: float32 [3], replicated, may hold values from -3 to 3
Outputs:
- next_fields: float32 [3, 512, 4096], P(None, 'gx', 'gy')
The draws below stay inside these ranges and needn't reach their ends.
All inputs are finite; a program needn't handle non-finite values.
Results may differ from the reference program's by a relative error of at most 0.0001.
Values sent between devices are 32-bit elements; how exact they have to be, the bound alone decides.
No kernel may reach another device: no remote copies, remote signals or barrier semaphores. Data moves between devices by JAX's collectives and lax.ppermute only.
A program may use at most 64 MiB of HBM per device.

```python
import math
import jax
import jax.numpy as jnp
from jax import lax

CX = 32
CY = 128
IN_CHANNELS = 3
C = 64
HID = 128
MODES_X = 8
MODES_Y = 8
STEPS = 2
LIFT_IN = 12
NX = 512
NY = 4096
N_GX = 16
N_GY = 32


def draw_fields(key, part):
    base = jax.random.fold_in(key, 17)
    rough_key, wave_key, column_key, phase_key, amplitude_key = jax.random.split(base, 5)
    terms = 6
    rows = jnp.arange(NX, dtype=jnp.int32)
    cols = jnp.arange(NY, dtype=jnp.int32)
    row_waves = jax.random.randint(wave_key, (IN_CHANNELS, terms), 1, 5)
    col_waves = jax.random.randint(column_key, (IN_CHANNELS, terms), -4, 5)
    phases = jax.random.uniform(phase_key, (IN_CHANNELS, terms), jnp.float32, 0.0, 2.0 * math.pi)
    amplitudes = jax.random.uniform(amplitude_key, (IN_CHANNELS, terms), jnp.float32, 0.4, 0.8)
    smooth = jnp.zeros((IN_CHANNELS, NX, NY), jnp.float32)
    for term in range(terms):
        row_phase = (row_waves[:, term][:, None] * rows[None, :] % NX).astype(jnp.float32) * (2.0 * math.pi / NX)
        col_phase = (col_waves[:, term][:, None] * cols[None, :] % NY).astype(jnp.float32) * (2.0 * math.pi / NY)
        smooth = smooth + amplitudes[:, term, None, None] * jnp.sin(row_phase[:, :, None] + col_phase[:, None, :] + phases[:, term, None, None])
    rough = jax.random.truncated_normal(rough_key, -4.0, 4.0, (IN_CHANNELS, NX, NY), jnp.float32)
    return rough + smooth


def scatter_about(key, dims, deviation, most, held_as=jnp.bfloat16):
    result = deviation * jax.random.normal(key, dims, jnp.float32)
    return jnp.clip(result, min=-most, max=most).astype(held_as)


def setup_inputs(seed: int = 0) -> dict:
    seeds = jax.random.split(jax.random.key(seed), 13)
    return {
        "fields": draw_fields(jax.random.fold_in(seeds[12], 71), 0),
        "lift_weight": scatter_about(seeds[1], (LIFT_IN, C), LIFT_IN ** -0.5, 1.75, jnp.float32),
        "lift_bias": scatter_about(seeds[2], (C,), 0.5, 3.0, jnp.float32),
        "spectral_weight": scatter_about(seeds[3], (2, MODES_X, MODES_Y, C, C), (0.0055 * (CX * CY) ** 0.5), 4.0, jnp.float32),
        "bypass_weight": scatter_about(seeds[4], (C, C), C ** -0.5, 0.75, jnp.float32),
        "layer_bias": scatter_about(seeds[5], (C,), 0.5, 3.0, jnp.float32),
        "mlp_in_weight": scatter_about(seeds[6], (C, HID), C ** -0.5, 0.75, jnp.float32),
        "mlp_in_bias": scatter_about(seeds[7], (HID,), 0.5, 3.0, jnp.float32),
        "mlp_out_weight": scatter_about(seeds[8], (HID, C), HID ** -0.5, 0.5, jnp.float32),
        "mlp_out_bias": scatter_about(seeds[9], (C,), 0.5, 3.0, jnp.float32),
        "project_weight": scatter_about(seeds[10], (C, IN_CHANNELS), C ** -0.5, 0.75, jnp.float32),
        "project_bias": scatter_about(seeds[11], (IN_CHANNELS,), 0.5, 3.0, jnp.float32),
    }


HIGHEST_PRECISION = lax.Precision.HIGHEST


def pointwise(weights, inputs, biases):
    return jnp.einsum("io,ixy->oxy", weights, inputs, precision=HIGHEST_PRECISION) + biases[:, None, None]


def context_window(extent, tile_length, factor):
    positions = jnp.arange(extent, dtype=jnp.int32)
    anchor = (positions // tile_length) * (tile_length // factor) - (factor - 1) * (tile_length // (2 * factor))
    return ((anchor + positions % tile_length) % (extent // factor)).astype(jnp.int32)


def all_contexts(current):
    channels = current.shape[0]
    results = []
    for level_number in (1, 2, 3):
        factor = 2 ** level_number
        pooled = current.reshape(channels, NX // factor, factor, NY // factor, factor).mean(axis=(2, 4))
        rows_window = context_window(NX, CX, factor)
        cols_window = context_window(NY, CY, factor)
        results.append(jnp.take(jnp.take(pooled, rows_window, axis=1), cols_window, axis=2))
    return results


def spectral_tiles(hidden_tiles, spectral_weight):
    tile_rows = hidden_tiles.shape[2]
    tile_cols = hidden_tiles.shape[3]
    spectrum = jnp.fft.rfft2(hidden_tiles, axes=(2, 3))
    ordinal = jnp.arange(MODES_X, dtype=jnp.int32)
    rows_index = jnp.where(ordinal < MODES_X // 2, ordinal, ordinal + tile_rows - MODES_X)
    kept = spectrum[:, :, rows_index, :MODES_Y]
    complex_weight = spectral_weight[0] + 1j * spectral_weight[1]
    mixed_modes = jnp.einsum("gckj,kjco->gokj", kept, complex_weight, precision=HIGHEST_PRECISION)
    full_spectrum = jnp.zeros(spectrum.shape, spectrum.dtype).at[:, :, rows_index, :MODES_Y].set(mixed_modes)
    return jnp.fft.irfft2(full_spectrum, s=(tile_rows, tile_cols), axes=(2, 3))


def reference(fields, lift_weight, lift_bias, spectral_weight, bypass_weight, layer_bias, mlp_in_weight, mlp_in_bias, mlp_out_weight, mlp_out_bias, project_weight, project_bias):
    channels = fields.shape[0]
    hidden_width = lift_weight.shape[1]

    def slab_step(slab):
        hidden = pointwise(lift_weight, slab, lift_bias)
        tiles = hidden.reshape(hidden_width, CX, N_GY, CY).transpose(2, 0, 1, 3)
        spectral = spectral_tiles(tiles, spectral_weight).transpose(1, 2, 0, 3).reshape(hidden_width, CX, NY)
        mixed = jax.nn.gelu(spectral + pointwise(bypass_weight, hidden, layer_bias))
        inner = jax.nn.gelu(pointwise(mlp_in_weight, mixed, mlp_in_bias))
        refined = mixed + pointwise(mlp_out_weight, inner, mlp_out_bias)
        return slab[:channels] + pointwise(project_weight, refined, project_bias)

    current = fields
    for rollout in range(STEPS):
        features = jnp.concatenate([current] + all_contexts(current), axis=0)
        slabs = features.reshape(features.shape[0], N_GX, CX, NY).transpose(1, 0, 2, 3)
        updated = lax.map(slab_step, slabs)
        current = updated.transpose(1, 0, 2, 3).reshape(channels, NX, NY)
    return current
```

```python
import math

import jax
import jax.numpy as jnp
import numpy as np
from jax import lax
from jax.experimental import pallas as pl
from jax.experimental.pallas import tpu as pltpu
from jax.sharding import PartitionSpec as P

STEPS = 2
ROWS = 32
COLS = 128
FEATURES = 12
PADDED = 16
LANE_L3 = 64
LANE_L2 = 80
LANE_L3_COPY = 112

BF16 = jnp.bfloat16
F32 = jnp.float32
GELU_SCALE = math.sqrt(2.0 / math.pi)


def pool_tables():
    columns = np.zeros((COLS, 128), np.float32)
    for cell in range(COLS):
        columns[cell, cell // 2] = 0.5
        columns[cell, LANE_L2 + cell // 4] = 0.25
        columns[cell, LANE_L3 + cell // 8] = 0.125
        columns[cell, LANE_L3_COPY + cell // 8] = 0.125
    rows = np.zeros((96, 96), np.float32)
    for channel in range(3):
        for sub in range(8):
            for kind, (factor, row) in enumerate(
                [(2, sub), (2, sub + 8), (4, (sub + 4) % 8), (8, (sub + 2) % 4)]
            ):
                for inner in range(factor):
                    rows[channel * 32 + kind * 8 + sub, channel * 32 + row * factor + inner] = (
                        1.0 / factor
                    )
    return (
        np.concatenate([columns, columns], axis=0),
        np.concatenate([rows, rows], axis=1),
    )


def fourier_tables():
    signed = np.array([0, 1, 2, 3, -4, -3, -2, -1])
    theta = 2.0 * np.pi * ((signed[:, None] * np.arange(ROWS)[None, :]) % ROWS) / ROWS
    phi = 2.0 * np.pi * ((np.arange(8)[:, None] * np.arange(COLS)[None, :]) % COLS) / COLS
    forward_rows = np.zeros((256, ROWS * PADDED))
    for feature in range(FEATURES):
        for mode in range(8):
            for row in range(ROWS):
                forward_rows[feature * 8 + mode, row * PADDED + feature] = math.cos(
                    theta[mode, row]
                )
                forward_rows[128 + feature * 8 + mode, row * PADDED + feature] = -math.sin(
                    theta[mode, row]
                )
    forward_cols = np.concatenate([np.cos(phi), -np.sin(phi)], axis=0)
    inverse_rows = np.zeros((2, 8, 8, ROWS, 2, 8))
    for mode in range(8):
        for column in range(8):
            inverse_rows[0, mode, column, :, 0, column] = np.cos(theta[mode])
            inverse_rows[1, mode, column, :, 0, column] = -np.sin(theta[mode])
            inverse_rows[0, mode, column, :, 1, column] = np.sin(theta[mode])
            inverse_rows[1, mode, column, :, 1, column] = np.cos(theta[mode])
    weight = np.where(np.arange(8) == 0, 1.0, 2.0)[:, None] / (ROWS * COLS)
    inverse_cols = np.zeros((4, 8, 16, 2, COLS))
    for pair in range(4):
        for half in range(2):
            inverse_cols[pair, 2 * pair + half, :8, half] = weight * np.cos(phi)
            inverse_cols[pair, 2 * pair + half, 8:, half] = -weight * np.sin(phi)
    return (
        forward_rows,
        forward_cols,
        inverse_rows.reshape(128, 512),
        inverse_cols.reshape(4 * 128, 256),
    )


def halves_of_table(table):
    table = jnp.asarray(table.astype(np.float32))
    high = table.astype(BF16)
    low = (table - high.astype(F32)).astype(BF16)
    return high, low


def split(value):
    high = value.astype(BF16)
    return high, (value - high.astype(F32)).astype(BF16)


def matmul(left, right):
    return jnp.dot(left, right, preferred_element_type=F32)


def product(left, right):
    left_high, left_low = left
    right_high, right_low = right
    return (
        matmul(left_high, right_high) + matmul(left_high, right_low) + matmul(left_low, right_high)
    )


def gelu(value):
    inner = value * (GELU_SCALE + (GELU_SCALE * 0.044715) * (value * value))
    half = 0.5 * value
    return half + half * jnp.tanh(inner)


def pooled_blocks(flat, pool_columns, pool_rows):
    high, low = split(flat)
    across = matmul(jnp.concatenate([high, low], axis=1), pool_columns)
    high, low = split(across)
    pooled = matmul(pool_rows, jnp.concatenate([high, low], axis=0))
    lane = lax.broadcasted_iota(jnp.int32, (8, 128), 1)
    first = lane < LANE_L3
    second = (lane >= LANE_L2) & (lane < LANE_L3_COPY)
    upper = []
    lower = []
    for channel in range(3):
        base = channel * 32
        coarse = jnp.where(second, pooled[base + 16 : base + 24], pooled[base + 24 : base + 32])
        upper.append(jnp.where(first, pooled[base : base + 8], coarse))
        lower.append(jnp.where(first, pooled[base + 8 : base + 16], coarse))
    return upper, lower


def emit_slots(slots_ref, position, upper, lower):
    count = slots_ref.shape[0]
    for slot in range(count):
        ahead = lax.rem(slot - position + count, count) < count // 2
        for channel in range(3):
            slots_ref[slot, channel] = jnp.where(ahead, lower[channel], upper[channel])


def pool_kernel(current_ref, columns_ref, rows_ref, slots_ref, own_ref):
    flat = current_ref[...].reshape(96, 128)
    upper, lower = pooled_blocks(flat, columns_ref[...], rows_ref[...])
    for channel in range(3):
        own_ref[0, channel] = upper[channel]
        own_ref[1, channel] = lower[channel]
    emit_slots(slots_ref, lax.axis_index("gx"), upper, lower)


def strip_kernel(own_ref, got_ref, ready_ref, slots_ref, strip_ref):
    position = lax.axis_index("gx")
    lane = lax.broadcasted_iota(jnp.int32, (8, 128), 1)
    sub = lax.broadcasted_iota(jnp.int32, (8, 128), 0)
    first = lane < LANE_L3
    second = (lane >= LANE_L2) & (lane < LANE_L3_COPY)
    top = sub < 4
    low_two = sub < 2
    high_two = sub >= 6
    quarter = lane // 32

    upper_out = []
    lower_out = []
    for channel in range(3):
        near = {
            offset: got_ref[lax.rem(position + offset + 16, 16), channel]
            for offset in (-4, -3, -2, -1, 1, 2, 3, 4)
        }
        near[0] = own_ref[0, channel]
        finest = [near[-1], own_ref[0, channel], own_ref[1, channel], near[1]]
        middle = [(-2, -1), (-1, 0), (0, 1), (1, 2)]
        coarse = [(-4, -3, -2), (-2, -1, 0), (0, 1, 2), (2, 3, 4)]
        upper = jnp.zeros((8, 128), F32)
        lower = jnp.zeros((8, 128), F32)
        for block in range(4):
            before, after = middle[block]
            start, centre, end = coarse[block]
            wide = jnp.where(
                low_two, near[start], jnp.where(high_two, near[end], near[centre])
            )
            value = jnp.where(
                first,
                finest[block],
                jnp.where(second, jnp.where(top, near[before], near[after]), wide),
            )
            strip_ref[channel, block * 8 : block * 8 + 8] = value
            here = quarter == block
            upper = jnp.where(here, pltpu.roll(value, (32 * block - 64) % 128, 1), upper)
            lower = jnp.where(here, pltpu.roll(value, (32 * block - 96) % 128, 1), lower)
        upper_out.append(upper)
        lower_out.append(lower)
    emit_slots(slots_ref, lax.axis_index("gy"), upper_out, lower_out)


def stacked_left(value):
    high, low = split(value)
    return jnp.concatenate([high, high, low], axis=1)


def stacked_right(value):
    high, low = split(value)
    return jnp.concatenate([high, low, high], axis=0)


def prepare_kernel(
    lift_ref,
    lift_bias_ref,
    weight_ref,
    bypass_ref,
    layer_bias_ref,
    mlp_in_ref,
    mlp_in_bias_ref,
    mlp_out_ref,
    mlp_out_bias_ref,
    project_ref,
    project_bias_ref,
    mixing_ref,
    skip_ref,
    inner_ref,
    inner_bias_ref,
    last_ref,
    offset_ref,
):
    highest = lax.Precision.HIGHEST
    lift = jnp.concatenate(
        [lift_ref[...], lift_bias_ref[...], jnp.zeros((PADDED - FEATURES - 1, 64), F32)], axis=0
    )
    left = stacked_left(lift)

    def mode_step(mode, carry):
        both = jnp.concatenate([weight_ref[0, mode], weight_ref[1, mode]], axis=1)
        mixing_ref[pl.ds(mode, PADDED, stride=64), :] = matmul(left, stacked_right(both))
        return carry

    lax.fori_loop(0, 64, mode_step, 0, unroll=8)

    skip = jnp.dot(lift, bypass_ref[...], precision=highest)
    row = lax.broadcasted_iota(jnp.int32, skip.shape, 0)
    skip = skip + jnp.where(row == FEATURES, layer_bias_ref[...], 0.0)
    square = jnp.concatenate([skip, jnp.zeros((128 - PADDED, 64), F32)], axis=0)
    square = jnp.concatenate([square, jnp.zeros((128, 64), F32)], axis=1)
    skip_ref[...] = stacked_left(jnp.transpose(square)[:64, :PADDED])

    project = jnp.concatenate([project_ref[...], jnp.zeros((5, 64), F32)], axis=0)
    wide = jnp.concatenate([mlp_in_ref[...], jnp.zeros((64, 128), F32)], axis=0)
    inner = jnp.concatenate([jnp.transpose(wide)[:, :64], project], axis=0)
    inner_ref[...] = stacked_left(inner)
    inner_bias_ref[...] = jnp.transpose(jnp.broadcast_to(mlp_in_bias_ref[...], (128, 128)))
    last_ref[...] = stacked_left(jnp.dot(project, mlp_out_ref[...], precision=highest))
    sub = lax.broadcasted_iota(jnp.int32, (8, 3), 0)
    lane = lax.broadcasted_iota(jnp.int32, (8, 3), 1)
    constant = jnp.sum(project * mlp_out_bias_ref[...], axis=1, keepdims=True) + jnp.sum(
        jnp.where(sub == lane, project_bias_ref[...], 0.0), axis=1, keepdims=True
    )
    offset_ref[...] = jnp.broadcast_to(constant, (8, 128))


def contexts(strip_ref, before_ref, after_ref, got_ref, position, channel, block):
    lane = lax.broadcasted_iota(jnp.int32, (8, 128), 1)
    rows = slice(block * 8, block * 8 + 8)
    here = strip_ref[channel, rows]
    before = before_ref[channel, rows]
    after = after_ref[channel, rows]
    far = {
        offset: got_ref[lax.rem(position + offset + 32, 32), channel]
        for offset in (-4, -3, -2, 2, 3, 4)
    }
    packed = 32 * block

    def moved(value, source, target):
        shift = (target - source) % 128
        return value if shift == 0 else pltpu.roll(value, shift, 1)

    def gathered(pieces):
        result = moved(*pieces[-1][1:])
        for piece in reversed(pieces[:-1]):
            result = jnp.where(lane < piece[0], moved(*piece[1:]), result)
        return result

    first = gathered([(32, before, 32, 0), (96, here, 0, 32), (128, after, 0, 96)])
    second = gathered(
        [
            (16, far[-2], packed, 0),
            (48, before, LANE_L2, 16),
            (80, here, LANE_L2, 48),
            (112, after, LANE_L2, 80),
            (128, far[2], packed + 16, 112),
        ]
    )
    third = gathered(
        [
            (8, far[-4], packed + 24, 0),
            (24, far[-3], packed + 16, 8),
            (40, far[-2], packed + 16, 24),
            (56, before, LANE_L3, 40),
            (72, here, LANE_L3, 56),
            (88, after, LANE_L3, 72),
            (104, far[2], packed, 88),
            (120, far[3], packed, 104),
            (128, far[4], packed, 120),
        ]
    )
    return first, second, third


def tile_step(
    current_ref,
    strip_ref,
    before_ref,
    after_ref,
    got_ref,
    mixing_ref,
    skip_ref,
    inner_ref,
    inner_bias_ref,
    last_ref,
    offset_ref,
    rows_high_ref,
    rows_low_ref,
    cols_high_ref,
    cols_low_ref,
    back_rows_high_ref,
    back_rows_low_ref,
    back_cols_high_ref,
    back_cols_low_ref,
    features_ref,
    results_ref,
):
    position = lax.axis_index("gy")
    for channel in range(3):
        for block in range(4):
            pieces = (
                current_ref[channel, block * 8 : block * 8 + 8],
                *contexts(strip_ref, before_ref, after_ref, got_ref, position, channel, block),
            )
            for level in range(4):
                features_ref[
                    pl.ds(block * 8 * PADDED + level * 3 + channel, 8, stride=PADDED), :
                ] = pieces[level]
    for row in range(ROWS):
        tail = lax.broadcasted_iota(jnp.int32, (4, 128), 0)
        features_ref[row * PADDED + FEATURES : (row + 1) * PADDED, :] = jnp.where(
            tail == 0, 1.0, 0.0
        )

    features = split(features_ref[...])
    along_rows = product((rows_high_ref[...], rows_low_ref[...]), features)
    contract = (((1,), (1,)), ((), ()))
    along_high, along_low = split(along_rows)

    def transposed(left, right):
        return lax.dot_general(left, right, contract, preferred_element_type=F32)

    spectrum = (
        transposed(cols_high_ref[...], along_high)
        + transposed(cols_high_ref[...], along_low)
        + transposed(cols_low_ref[...], along_high)
    )
    real = spectrum[:8, :128] - spectrum[8:, 128:]
    imag = spectrum[8:, :128] + spectrum[:8, 128:]
    lane = lax.broadcasted_iota(jnp.int32, (8, 128), 1)
    sub = lax.broadcasted_iota(jnp.int32, (8, 128), 0)
    real = jnp.where(
        (lane == 8 * FEATURES) & (sub == 0), float(ROWS * COLS), jnp.where(lane < 96, real, 0.0)
    )
    modes = []
    sign = jnp.where(lane < 64, -1.0, 1.0)
    for mode in range(8):
        with_real = None
        with_imag = None
        for feature in range(FEATURES + (1 if mode == 0 else 0)):
            place = feature * 8 + mode
            weights = mixing_ref[feature * 64 + mode * 8 : feature * 64 + mode * 8 + 8, :]
            term = jnp.broadcast_to(real[:, place : place + 1], (8, 128)) * weights
            with_real = term if with_real is None else with_real + term
            if feature < FEATURES:
                term = jnp.broadcast_to(imag[:, place : place + 1], (8, 128)) * weights
                with_imag = term if with_imag is None else with_imag + term
        modes.append(with_real + sign * pltpu.roll(with_imag, 64, 1))
    turned = jnp.transpose(jnp.concatenate(modes, axis=0))
    outputs = split(jnp.concatenate([turned[:64], turned[64:]], axis=1))
    back = product(outputs, (back_rows_high_ref[...], back_rows_low_ref[...]))
    stacked = split(
        jnp.concatenate([back[:, 128 * block : 128 * block + 128] for block in range(4)], axis=0)
    )

    skip = skip_ref[...]
    inner_left = inner_ref[...]
    inner_bias = jnp.concatenate([inner_bias_ref[...], inner_bias_ref[...]], axis=1)
    last_left = last_ref[...]
    offset = jnp.concatenate([offset_ref[...], offset_ref[...]], axis=1)
    for pair in range(4):
        table = (
            back_cols_high_ref[pair * 128 : pair * 128 + 128, :],
            back_cols_low_ref[pair * 128 : pair * 128 + 128, :],
        )
        spectral = product(stacked, table)
        for block in range(4):
            row = block * 8 + pair * 2
            cells = jnp.concatenate(
                [
                    features_ref[row * PADDED : (row + 1) * PADDED, :],
                    features_ref[(row + 1) * PADDED : (row + 2) * PADDED, :],
                ],
                axis=1,
            )
            mixed = gelu(
                spectral[block * 64 : block * 64 + 64] + matmul(skip, stacked_right(cells))
            )
            wide = matmul(inner_left, stacked_right(mixed))
            hidden = gelu(wide[:128] + inner_bias)
            total = wide[128:136] + offset + matmul(last_left, stacked_right(hidden))
            results_ref[row * 8 : row * 8 + 8, :] = total[:, :128]
            results_ref[(row + 1) * 8 : (row + 2) * 8, :] = total[:, 128:]
    return [
        current_ref[channel]
        + results_ref[pl.ds(channel, ROWS, stride=8), :]
        for channel in range(3)
    ]


def final_kernel(*refs):
    inputs, next_ref, scratch = refs[:19], refs[19], refs[20:]
    updated = tile_step(*inputs, *scratch)
    for channel in range(3):
        next_ref[channel] = updated[channel]


def middle_kernel(*refs):
    inputs, columns_ref, rows_ref = refs[:19], refs[19], refs[20]
    next_ref, slots_ref, own_ref = refs[21:24]
    updated = tile_step(*inputs, *refs[24:])
    for channel in range(3):
        next_ref[channel] = updated[channel]
    upper, lower = pooled_blocks(
        jnp.concatenate(updated, axis=0), columns_ref[...], rows_ref[...]
    )
    for channel in range(3):
        own_ref[0, channel] = upper[channel]
        own_ref[1, channel] = lower[channel]
    emit_slots(slots_ref, lax.axis_index("gx"), upper, lower)


VMEM = pl.BlockSpec(memory_space=pltpu.VMEM)


def resident(operand):
    return pltpu.with_memory_space_constraint(operand, pltpu.VMEM)


def call(body, name, operands, results, scratch=()):
    return pl.pallas_call(
        body,
        name=name,
        out_shape=[pltpu.VMEM(*(r if isinstance(r[0], tuple) else (r, F32))) for r in results],
        in_specs=[VMEM] * len(operands),
        out_specs=[VMEM] * len(results),
        scratch_shapes=list(scratch),
        compiler_params=pltpu.CompilerParams(vmem_limit_bytes=16 << 20),
    )(
        *(
            operand if operand.ndim == 4 and operand.shape[1] == 64 else resident(operand)
            for operand in operands
        )
    )


def shards(
    fields,
    lift_weight,
    lift_bias,
    spectral_weight,
    bypass_weight,
    layer_bias,
    mlp_in_weight,
    mlp_in_bias,
    mlp_out_weight,
    mlp_out_bias,
    project_weight,
    project_bias,
):
    n_gx = lax.axis_size("gx")
    n_gy = lax.axis_size("gy")
    pool_columns, pool_rows = (jnp.asarray(table).astype(BF16) for table in pool_tables())
    tables = [half for table in fourier_tables() for half in halves_of_table(table)]

    block = (3, 8, 128)
    slots_x, own = call(
        pool_kernel, "pool", [fields, pool_columns, pool_rows], [(n_gx, *block), (2, *block)]
    )
    prepared = call(
        prepare_kernel,
        "prepare",
        [
            lift_weight,
            lift_bias[None],
            spectral_weight.reshape(2, 64, 64, 64),
            bypass_weight,
            layer_bias[None],
            mlp_in_weight,
            mlp_in_bias[None],
            mlp_out_weight.T,
            mlp_out_bias[None],
            project_weight.T,
            project_bias[None],
        ],
        [
            (PADDED * 64, 128),
            ((64, 3 * PADDED), BF16),
            ((136, 192), BF16),
            (128, 128),
            ((8, 384), BF16),
            (8, 128),
        ],
    )

    forward = [(i, (i + 1) % n_gy) for i in range(n_gy)]
    backward = [((i + 1) % n_gy, i) for i in range(n_gy)]
    current = fields
    for step in range(STEPS):
        got_x = lax.all_to_all(slots_x, "gx", 0, 0, tiled=True)
        slots_y, strip = call(
            strip_kernel, "strip", [own, got_x, prepared[-1]], [(n_gy, *block), (3, ROWS, 128)]
        )
        got_y = lax.all_to_all(slots_y, "gy", 0, 0, tiled=True)
        before = lax.ppermute(strip, "gy", forward)
        after = lax.ppermute(strip, "gy", backward)
        operands = [
            current,
            strip,
            before,
            after,
            got_y,
            *prepared,
            *tables,
        ]
        scratch = [pltpu.VMEM((ROWS * PADDED, 128), F32), pltpu.VMEM((ROWS * 8, 128), F32)]
        if step + 1 < STEPS:
            current, slots_x, own = call(
                middle_kernel,
                "middle",
                [*operands, pool_columns, pool_rows],
                [fields.shape, (n_gx, *block), (2, *block)],
                scratch,
            )
        else:
            (current,) = call(final_kernel, "final", operands, [fields.shape], scratch)
    return current


def solution(mesh):
    placed = (P(None, "gx", "gy"), P(), P(), P(), P(), P(), P(), P(), P(), P(), P(), P())
    return jax.shard_map(
        shards, mesh=mesh, in_specs=placed, out_specs=P(None, "gx", "gy"), check_vma=False
    )
```

```python
import math

import jax
import jax.numpy as jnp
import numpy as np
from jax import lax
from jax.experimental import pallas as pl
from jax.experimental.pallas import tpu as pltpu
from jax.sharding import PartitionSpec as P

STEPS = 2
ROWS = 32
COLS = 128
FEATURES = 12
PADDED = 16
LANE_L3 = 64
LANE_L2 = 80
LANE_L3_COPY = 112

BF16 = jnp.bfloat16
F32 = jnp.float32
GELU_SCALE = math.sqrt(2.0 / math.pi)


def pool_tables():
    cell = lax.broadcasted_iota(jnp.int32, (COLS, 128), 0)
    lane = lax.broadcasted_iota(jnp.int32, (COLS, 128), 1)
    eighth = cell >> 3
    columns = jnp.where(
        lane < LANE_L3,
        jnp.where(cell >> 1 == lane, 0.5, 0.0),
        jnp.where(
            (lane >= LANE_L2) & (lane < LANE_L3_COPY),
            jnp.where(cell >> 2 == lane - LANE_L2, 0.25, 0.0),
            jnp.where(
                (eighth == lane - LANE_L3) | (eighth == lane - LANE_L3_COPY), 0.125, 0.0
            ),
        ),
    ).astype(BF16)
    out = lax.broadcasted_iota(jnp.int32, (96, 96), 0)
    cell = lax.broadcasted_iota(jnp.int32, (96, 96), 1)
    kind = (out >> 3) & 3
    sub = out & 7
    row = cell & 31
    fine = jnp.where(row >> 1 == sub + 8 * kind, 0.5, 0.0)
    middle = jnp.where(row >> 2 == ((sub + 4) & 7), 0.25, 0.0)
    coarse = jnp.where(row >> 3 == ((sub + 2) & 3), 0.125, 0.0)
    rows = jnp.where(kind < 2, fine, jnp.where(kind == 2, middle, coarse))
    rows = jnp.where(out >> 5 == cell >> 5, rows, 0.0).astype(BF16)
    return jnp.concatenate([columns, columns], axis=0), jnp.concatenate([rows, rows], axis=1)


def fourier_tables():
    signed = np.array([0, 1, 2, 3, -4, -3, -2, -1])
    theta = 2.0 * np.pi * ((signed[:, None] * np.arange(ROWS)[None, :]) % ROWS) / ROWS
    phi = 2.0 * np.pi * ((np.arange(8)[:, None] * np.arange(COLS)[None, :]) % COLS) / COLS
    forward_rows = np.zeros((256, ROWS * PADDED))
    for feature in range(FEATURES):
        for mode in range(8):
            for row in range(ROWS):
                forward_rows[feature * 8 + mode, row * PADDED + feature] = math.cos(
                    theta[mode, row]
                )
                forward_rows[128 + feature * 8 + mode, row * PADDED + feature] = -math.sin(
                    theta[mode, row]
                )
    forward_cols = np.concatenate([np.cos(phi), -np.sin(phi)], axis=0)
    inverse_rows = np.zeros((2, 8, 8, ROWS, 2, 8))
    for mode in range(8):
        for column in range(8):
            inverse_rows[0, mode, column, :, 0, column] = np.cos(theta[mode])
            inverse_rows[1, mode, column, :, 0, column] = -np.sin(theta[mode])
            inverse_rows[0, mode, column, :, 1, column] = np.sin(theta[mode])
            inverse_rows[1, mode, column, :, 1, column] = np.cos(theta[mode])
    weight = np.where(np.arange(8) == 0, 1.0, 2.0)[:, None] / (ROWS * COLS)
    inverse_cols = np.zeros((4, 8, 16, 2, COLS))
    for pair in range(4):
        for half in range(2):
            inverse_cols[pair, 2 * pair + half, :8, half] = 0.5 * weight * np.cos(phi)
            inverse_cols[pair, 2 * pair + half, 8:, half] = -0.5 * weight * np.sin(phi)
    return (
        forward_rows,
        forward_cols,
        inverse_rows.reshape(128, 512),
        inverse_cols.reshape(4 * 128, 256),
    )


def halves_of_table(table):
    table = jnp.asarray(table.astype(np.float32))
    high = table.astype(BF16)
    low = (table - high.astype(F32)).astype(BF16)
    return high, low


def split(value):
    high = value.astype(BF16)
    return high, (value - high.astype(F32)).astype(BF16)


def matmul(left, right):
    return jnp.dot(left, right, preferred_element_type=F32)


def product(left, right):
    left_high, left_low = left
    right_high, right_low = right
    return (
        matmul(left_high, right_high) + matmul(left_high, right_low) + matmul(left_low, right_high)
    )


def gelu_of_double(half):
    inner = half * (2.0 * GELU_SCALE + (8.0 * GELU_SCALE * 0.044715) * (half * half))
    return half + half * jnp.tanh(inner)


def pooled_blocks(flat):
    pool_columns, pool_rows = pool_tables()
    high, low = split(flat)
    across = matmul(jnp.concatenate([high, low], axis=1), pool_columns)
    high, low = split(across)
    pooled = matmul(pool_rows, jnp.concatenate([high, low], axis=0))
    lane = lax.broadcasted_iota(jnp.int32, (8, 128), 1)
    first = lane < LANE_L3
    second = (lane >= LANE_L2) & (lane < LANE_L3_COPY)
    upper = []
    lower = []
    for channel in range(3):
        base = channel * 32
        coarse = jnp.where(second, pooled[base + 16 : base + 24], pooled[base + 24 : base + 32])
        upper.append(jnp.where(first, pooled[base : base + 8], coarse))
        lower.append(jnp.where(first, pooled[base + 8 : base + 16], coarse))
    return upper, lower


def emit_slots(slots_ref, position, upper, lower):
    count = slots_ref.shape[0]
    for slot in range(count):
        ahead = lax.rem(slot - position + count, count) < count // 2
        for channel in range(3):
            slots_ref[slot, channel] = jnp.where(ahead, lower[channel], upper[channel])


def pool_kernel(current_ref, slots_ref, own_ref):
    flat = current_ref[...].reshape(96, 128)
    upper, lower = pooled_blocks(flat)
    for channel in range(3):
        own_ref[0, channel] = upper[channel]
        own_ref[1, channel] = lower[channel]
    emit_slots(slots_ref, lax.axis_index("gx"), upper, lower)


def strip_kernel(own_ref, got_ref, ready_ref, slots_ref, strip_ref):
    position = lax.axis_index("gx")
    lane = lax.broadcasted_iota(jnp.int32, (8, 128), 1)
    sub = lax.broadcasted_iota(jnp.int32, (8, 128), 0)
    first = lane < LANE_L3
    second = (lane >= LANE_L2) & (lane < LANE_L3_COPY)
    top = sub < 4
    low_two = sub < 2
    high_two = sub >= 6
    quarter = lane // 32

    upper_out = []
    lower_out = []
    for channel in range(3):
        near = {
            offset: got_ref[lax.rem(position + offset + 16, 16), channel]
            for offset in (-4, -3, -2, -1, 1, 2, 3, 4)
        }
        near[0] = own_ref[0, channel]
        finest = [near[-1], own_ref[0, channel], own_ref[1, channel], near[1]]
        middle = [(-2, -1), (-1, 0), (0, 1), (1, 2)]
        coarse = [(-4, -3, -2), (-2, -1, 0), (0, 1, 2), (2, 3, 4)]
        upper = jnp.zeros((8, 128), F32)
        lower = jnp.zeros((8, 128), F32)
        for block in range(4):
            before, after = middle[block]
            start, centre, end = coarse[block]
            wide = jnp.where(
                low_two, near[start], jnp.where(high_two, near[end], near[centre])
            )
            value = jnp.where(
                first,
                finest[block],
                jnp.where(second, jnp.where(top, near[before], near[after]), wide),
            )
            strip_ref[channel, block * 8 : block * 8 + 8] = value
            here = quarter == block
            upper = jnp.where(here, pltpu.roll(value, (32 * block - 64) % 128, 1), upper)
            lower = jnp.where(here, pltpu.roll(value, (32 * block - 96) % 128, 1), lower)
        upper_out.append(upper)
        lower_out.append(lower)
    emit_slots(slots_ref, lax.axis_index("gy"), upper_out, lower_out)


def stacked_left(value):
    high, low = split(value)
    return jnp.concatenate([high, high, low], axis=1)


def stacked_right(value):
    high, low = split(value)
    return jnp.concatenate([high, low, high], axis=0)


def prepare_kernel(
    lift_ref,
    lift_bias_ref,
    weight_ref,
    bypass_ref,
    layer_bias_ref,
    mlp_in_ref,
    mlp_in_bias_ref,
    mlp_out_ref,
    mlp_out_bias_ref,
    project_ref,
    project_bias_ref,
    mixing_ref,
    skip_ref,
    inner_ref,
    inner_bias_ref,
    last_ref,
    offset_ref,
):
    highest = lax.Precision.HIGHEST
    lift = jnp.concatenate(
        [lift_ref[...], lift_bias_ref[...], jnp.zeros((PADDED - FEATURES - 1, 64), F32)], axis=0
    )
    left = stacked_left(lift)

    def mode_step(mode, carry):
        both = jnp.concatenate([weight_ref[0, mode], weight_ref[1, mode]], axis=1)
        mixing_ref[pl.ds(mode, PADDED, stride=64), :] = matmul(left, stacked_right(both))
        return carry

    lax.fori_loop(0, 64, mode_step, 0, unroll=8)

    skip = jnp.dot(lift, bypass_ref[...], precision=highest)
    row = lax.broadcasted_iota(jnp.int32, skip.shape, 0)
    skip = skip + jnp.where(row == FEATURES, layer_bias_ref[...], 0.0)
    square = jnp.concatenate([0.5 * skip, jnp.zeros((128 - PADDED, 64), F32)], axis=0)
    square = jnp.concatenate([square, jnp.zeros((128, 64), F32)], axis=1)
    skip_ref[...] = stacked_left(jnp.transpose(square)[:64, :PADDED])

    project = jnp.concatenate([project_ref[...], jnp.zeros((5, 64), F32)], axis=0)
    wide = jnp.concatenate([mlp_in_ref[...], jnp.zeros((64, 128), F32)], axis=0)
    inner = jnp.concatenate([0.5 * jnp.transpose(wide)[:, :64], project], axis=0)
    inner_ref[...] = stacked_left(inner)
    inner_bias_ref[...] = jnp.transpose(
        jnp.broadcast_to(0.5 * mlp_in_bias_ref[...], (128, 128))
    )
    last = jnp.dot(project, mlp_out_ref[...], precision=highest)
    for channel in range(3):
        last_ref[channel] = jnp.transpose(
            jnp.broadcast_to(last[channel : channel + 1], (128, 128))
        )
    sub = lax.broadcasted_iota(jnp.int32, (8, 3), 0)
    lane = lax.broadcasted_iota(jnp.int32, (8, 3), 1)
    constant = jnp.sum(project * mlp_out_bias_ref[...], axis=1, keepdims=True) + jnp.sum(
        jnp.where(sub == lane, project_bias_ref[...], 0.0), axis=1, keepdims=True
    )
    offset_ref[...] = jnp.broadcast_to(constant, (8, 128))


def contexts(strip_ref, twin_ref, other_ref, got_ref, position, channel, block):
    lane = lax.broadcasted_iota(jnp.int32, (8, 128), 1)
    rows = slice(block * 8, block * 8 + 8)
    here = strip_ref[channel, rows]
    twin = twin_ref[channel, rows]
    other = other_ref[channel, rows]
    even = position % 2 == 0
    before = jnp.where(even, other, twin)
    after = jnp.where(even, twin, other)
    far = {
        offset: got_ref[lax.rem(position + offset + 32, 32), channel]
        for offset in (-4, -3, -2, 2, 3, 4)
    }
    packed = 32 * block

    def moved(value, source, target):
        shift = (target - source) % 128
        return value if shift == 0 else pltpu.roll(value, shift, 1)

    def gathered(pieces):
        result = moved(*pieces[-1][1:])
        for piece in reversed(pieces[:-1]):
            result = jnp.where(lane < piece[0], moved(*piece[1:]), result)
        return result

    first = gathered([(32, before, 32, 0), (96, here, 0, 32), (128, after, 0, 96)])
    second = gathered(
        [
            (16, far[-2], packed, 0),
            (48, before, LANE_L2, 16),
            (80, here, LANE_L2, 48),
            (112, after, LANE_L2, 80),
            (128, far[2], packed + 16, 112),
        ]
    )
    third = gathered(
        [
            (8, far[-4], packed + 24, 0),
            (24, far[-3], packed + 16, 8),
            (40, far[-2], packed + 16, 24),
            (56, before, LANE_L3, 40),
            (72, here, LANE_L3, 56),
            (88, after, LANE_L3, 72),
            (104, far[2], packed, 88),
            (120, far[3], packed, 104),
            (128, far[4], packed, 120),
        ]
    )
    return first, second, third


def tile_step(
    current_ref,
    strip_ref,
    twin_ref,
    other_ref,
    got_ref,
    mixing_ref,
    skip_ref,
    inner_ref,
    inner_bias_ref,
    last_ref,
    offset_ref,
    rows_high_ref,
    rows_low_ref,
    cols_high_ref,
    cols_low_ref,
    back_rows_high_ref,
    back_rows_low_ref,
    back_cols_high_ref,
    back_cols_low_ref,
    features_ref,
    results_ref,
    partial_ref,
):
    position = lax.axis_index("gy")
    for channel in range(3):
        for block in range(4):
            pieces = (
                current_ref[channel, block * 8 : block * 8 + 8],
                *contexts(strip_ref, twin_ref, other_ref, got_ref, position, channel, block),
            )
            for level in range(4):
                features_ref[
                    pl.ds(block * 8 * PADDED + level * 3 + channel, 8, stride=PADDED), :
                ] = pieces[level]
    for row in range(ROWS):
        tail = lax.broadcasted_iota(jnp.int32, (4, 128), 0)
        features_ref[row * PADDED + FEATURES : (row + 1) * PADDED, :] = jnp.where(
            tail == 0, 1.0, 0.0
        )

    features = split(features_ref[...])
    along_rows = product((rows_high_ref[...], rows_low_ref[...]), features)
    contract = (((1,), (1,)), ((), ()))
    along_high, along_low = split(along_rows)

    def transposed(left, right):
        return lax.dot_general(left, right, contract, preferred_element_type=F32)

    spectrum = (
        transposed(cols_high_ref[...], along_high)
        + transposed(cols_high_ref[...], along_low)
        + transposed(cols_low_ref[...], along_high)
    )
    real = spectrum[:8, :128] - spectrum[8:, 128:]
    imag = spectrum[8:, :128] + spectrum[:8, 128:]
    lane = lax.broadcasted_iota(jnp.int32, (8, 128), 1)
    sub = lax.broadcasted_iota(jnp.int32, (8, 128), 0)
    real = jnp.where(
        (lane == 8 * FEATURES) & (sub == 0), float(ROWS * COLS), jnp.where(lane < 96, real, 0.0)
    )
    modes = []
    sign = jnp.where(lane < 64, -1.0, 1.0)
    for mode in range(8):
        with_real = None
        with_imag = None
        for feature in range(FEATURES + (1 if mode == 0 else 0)):
            place = feature * 8 + mode
            weights = mixing_ref[feature * 64 + mode * 8 : feature * 64 + mode * 8 + 8, :]
            term = jnp.broadcast_to(real[:, place : place + 1], (8, 128)) * weights
            with_real = term if with_real is None else with_real + term
            if feature < FEATURES:
                term = jnp.broadcast_to(imag[:, place : place + 1], (8, 128)) * weights
                with_imag = term if with_imag is None else with_imag + term
        modes.append(with_real + sign * pltpu.roll(with_imag, 64, 1))
    turned = jnp.transpose(jnp.concatenate(modes, axis=0))
    outputs = split(jnp.concatenate([turned[:64], turned[64:]], axis=1))
    back = product(outputs, (back_rows_high_ref[...], back_rows_low_ref[...]))
    stacked = split(
        jnp.concatenate([back[:, 128 * block : 128 * block + 128] for block in range(4)], axis=0)
    )

    skip = skip_ref[...]
    inner_left = inner_ref[...]
    inner_bias = jnp.concatenate([inner_bias_ref[...], inner_bias_ref[...]], axis=1)
    offset = jnp.concatenate([offset_ref[...], offset_ref[...]], axis=1)
    for pair in range(4):
        table = (
            back_cols_high_ref[pair * 128 : pair * 128 + 128, :],
            back_cols_low_ref[pair * 128 : pair * 128 + 128, :],
        )
        spectral = product(stacked, table)
        for block in range(4):
            row = block * 8 + pair * 2
            cells = jnp.concatenate(
                [
                    features_ref[row * PADDED : (row + 1) * PADDED, :],
                    features_ref[(row + 1) * PADDED : (row + 2) * PADDED, :],
                ],
                axis=1,
            )
            mixed = gelu_of_double(
                spectral[block * 64 : block * 64 + 64] + matmul(skip, stacked_right(cells))
            )
            wide = matmul(inner_left, stacked_right(mixed))
            hidden = gelu_of_double(wide[:128] + inner_bias)
            total = wide[128:136] + offset
            for half in range(2):
                lanes = slice(half * 128, half * 128 + 128)
                results_ref[(row + half) * 8 : (row + half) * 8 + 8, :] = total[:, lanes]
                for channel in range(3):
                    partial = None
                    for start in range(0, 128, 8):
                        term = hidden[start : start + 8, lanes] * last_ref[
                            channel, start : start + 8
                        ]
                        partial = term if partial is None else partial + term
                    partial_ref[channel, (row + half) * 8 : (row + half) * 8 + 8] = partial

    def sublane_sum(channel):
        total = results_ref[pl.ds(channel, ROWS, stride=8), :]
        for sub in range(8):
            total = total + partial_ref[channel, pl.ds(sub, ROWS, stride=8), :]
        return total

    return [current_ref[channel] + sublane_sum(channel) for channel in range(3)]


def final_kernel(*refs):
    next_ref = refs[19]
    updated = tile_step(*refs[:19], *refs[20:])
    for channel in range(3):
        next_ref[channel] = updated[channel]


def middle_kernel(*refs):
    next_ref, slots_ref, own_ref = refs[19:22]
    updated = tile_step(*refs[:19], *refs[22:])
    for channel in range(3):
        next_ref[channel] = updated[channel]
    upper, lower = pooled_blocks(jnp.concatenate(updated, axis=0))
    for channel in range(3):
        own_ref[0, channel] = upper[channel]
        own_ref[1, channel] = lower[channel]
    emit_slots(slots_ref, lax.axis_index("gx"), upper, lower)


VMEM = pl.BlockSpec(memory_space=pltpu.VMEM)


def resident(operand):
    return pltpu.with_memory_space_constraint(operand, pltpu.VMEM)


def call(body, name, operands, results, scratch=()):
    return pl.pallas_call(
        body,
        name=name,
        out_shape=[pltpu.VMEM(*(r if isinstance(r[0], tuple) else (r, F32))) for r in results],
        in_specs=[VMEM] * len(operands),
        out_specs=[VMEM] * len(results),
        scratch_shapes=list(scratch),
        compiler_params=pltpu.CompilerParams(vmem_limit_bytes=16 << 20),
    )(
        *(
            operand if operand.ndim == 4 and operand.shape[1] == 64 else resident(operand)
            for operand in operands
        )
    )


def shards(
    fields,
    lift_weight,
    lift_bias,
    spectral_weight,
    bypass_weight,
    layer_bias,
    mlp_in_weight,
    mlp_in_bias,
    mlp_out_weight,
    mlp_out_bias,
    project_weight,
    project_bias,
):
    n_gx = lax.axis_size("gx")
    n_gy = lax.axis_size("gy")
    tables = [half for table in fourier_tables() for half in halves_of_table(table)]

    block = (3, 8, 128)
    slots_x, own = call(
        pool_kernel, "pool", [fields], [(n_gx, *block), (2, *block)]
    )
    prepared = call(
        prepare_kernel,
        "prepare",
        [
            lift_weight,
            lift_bias[None],
            spectral_weight.reshape(2, 64, 64, 64),
            bypass_weight,
            layer_bias[None],
            mlp_in_weight,
            mlp_in_bias[None],
            mlp_out_weight.T,
            mlp_out_bias[None],
            project_weight.T,
            project_bias[None],
        ],
        [
            (PADDED * 64, 128),
            ((64, 3 * PADDED), BF16),
            ((136, 192), BF16),
            (128, 128),
            (3, 128, 128),
            (8, 128),
        ],
    )

    twins = [(i, i ^ 1) for i in range(n_gy)]
    others = [(i, (i + 1 if i % 2 else i - 1) % n_gy) for i in range(n_gy)]
    current = fields
    for step in range(STEPS):
        got_x = lax.all_to_all(slots_x, "gx", 0, 0, tiled=True)
        slots_y, strip = call(
            strip_kernel, "strip", [own, got_x, prepared[-1]], [(n_gy, *block), (3, ROWS, 128)]
        )
        got_y = lax.all_to_all(slots_y, "gy", 0, 0, tiled=True)
        twin = lax.ppermute(strip, "gy", twins)
        other = lax.ppermute(strip, "gy", others)
        operands = [
            current,
            strip,
            twin,
            other,
            got_y,
            *prepared,
            *tables,
        ]
        scratch = [pltpu.VMEM((ROWS * PADDED, 128), F32), pltpu.VMEM((ROWS * 8, 128), F32), pltpu.VMEM((3, ROWS * 8, 128), F32)]
        if step + 1 < STEPS:
            current, slots_x, own = call(
                middle_kernel,
                "middle",
                operands,
                [fields.shape, (n_gx, *block), (2, *block)],
                scratch,
            )
        else:
            (current,) = call(final_kernel, "final", operands, [fields.shape], scratch)
    return current


def solution(mesh):
    placed = (P(None, "gx", "gy"), P(), P(), P(), P(), P(), P(), P(), P(), P(), P(), P())
    return jax.shard_map(
        shards, mesh=mesh, in_specs=placed, out_specs=P(None, "gx", "gy"), check_vma=False
    )
```

```python
import math

import jax
import jax.numpy as jnp
import numpy as np
from jax import lax
from jax.experimental import pallas as pl
from jax.experimental.pallas import tpu as pltpu
from jax.sharding import PartitionSpec as P

STEPS = 2
ROWS = 32
COLS = 128
FEATURES = 12
PADDED = 16
LANE_L3 = 64
LANE_L2 = 80
LANE_L3_COPY = 112

BF16 = jnp.bfloat16
F32 = jnp.float32
GELU_SCALE = math.sqrt(2.0 / math.pi)


def refill_tables():
    columns = np.zeros((128, 256), np.float32)
    for cell in range(64):
        columns[cell, LANE_L2 + cell // 2] = 0.5
        columns[cell, LANE_L3 + cell // 4] = 0.25
        columns[cell, LANE_L3_COPY + cell // 4] = 0.25
    for cell in range(32):
        columns[64 + cell, 128 + LANE_L2 + cell] = 1.0
        columns[64 + cell, 128 + LANE_L3 + cell // 2] = 0.5
        columns[64 + cell, 128 + LANE_L3_COPY + cell // 2] = 0.5
    rows = np.zeros((96, 96), np.float32)
    for side in range(2):
        for channel in range(3):
            base = side * 24 + channel * 8
            for sub in range(8):
                row = (sub + 4) % 8
                if (row >= 4) == (side == 0):
                    start = base + 2 * (row % 4)
                    rows[base + sub, start : start + 2] = 0.5
                else:
                    rows[base + sub, 48 + base + sub] = 1.0
                row = (sub + 2) % 4
                if (row >= 2) == (side == 0):
                    start = base + 4 * (row % 2)
                    rows[48 + base + sub, start : start + 4] = 0.25
                else:
                    start = 48 + base + (2 * row + 4) % 8
                    rows[48 + base + sub, start : start + 2] = 0.5
    return np.concatenate([columns, columns], axis=0), np.concatenate([rows, rows], axis=1)


def pool_tables():
    cell = lax.broadcasted_iota(jnp.int32, (COLS, 128), 0)
    lane = lax.broadcasted_iota(jnp.int32, (COLS, 128), 1)
    eighth = cell >> 3
    columns = jnp.where(
        lane < LANE_L3,
        jnp.where(cell >> 1 == lane, 0.5, 0.0),
        jnp.where(
            (lane >= LANE_L2) & (lane < LANE_L3_COPY),
            jnp.where(cell >> 2 == lane - LANE_L2, 0.25, 0.0),
            jnp.where(
                (eighth == lane - LANE_L3) | (eighth == lane - LANE_L3_COPY), 0.125, 0.0
            ),
        ),
    ).astype(BF16)
    out = lax.broadcasted_iota(jnp.int32, (96, 96), 0)
    cell = lax.broadcasted_iota(jnp.int32, (96, 96), 1)
    kind = (out >> 3) & 3
    sub = out & 7
    row = cell & 31
    fine = jnp.where(row >> 1 == sub + 8 * kind, 0.5, 0.0)
    middle = jnp.where(row >> 2 == ((sub + 4) & 7), 0.25, 0.0)
    coarse = jnp.where(row >> 3 == ((sub + 2) & 3), 0.125, 0.0)
    rows = jnp.where(kind < 2, fine, jnp.where(kind == 2, middle, coarse))
    rows = jnp.where(out >> 5 == cell >> 5, rows, 0.0).astype(BF16)
    return jnp.concatenate([columns, columns], axis=0), jnp.concatenate([rows, rows], axis=1)


def fourier_tables():
    signed = np.array([0, 1, 2, 3, -4, -3, -2, -1])
    theta = 2.0 * np.pi * ((signed[:, None] * np.arange(ROWS)[None, :]) % ROWS) / ROWS
    phi = 2.0 * np.pi * ((np.arange(8)[:, None] * np.arange(COLS)[None, :]) % COLS) / COLS
    forward_rows = np.zeros((256, ROWS * PADDED))
    for feature in range(FEATURES):
        for mode in range(8):
            for row in range(ROWS):
                forward_rows[feature * 8 + mode, row * PADDED + feature] = math.cos(
                    theta[mode, row]
                )
                forward_rows[128 + feature * 8 + mode, row * PADDED + feature] = -math.sin(
                    theta[mode, row]
                )
    forward_cols = np.concatenate([np.cos(phi), -np.sin(phi)], axis=0)
    inverse_rows = np.zeros((2, 8, 8, ROWS, 2, 8))
    for mode in range(8):
        for column in range(8):
            inverse_rows[0, mode, column, :, 0, column] = np.cos(theta[mode])
            inverse_rows[1, mode, column, :, 0, column] = -np.sin(theta[mode])
            inverse_rows[0, mode, column, :, 1, column] = np.sin(theta[mode])
            inverse_rows[1, mode, column, :, 1, column] = np.cos(theta[mode])
    weight = np.where(np.arange(8) == 0, 1.0, 2.0)[:, None] / (ROWS * COLS)
    inverse_cols = np.zeros((4, 8, 16, 2, COLS))
    for pair in range(4):
        for half in range(2):
            inverse_cols[pair, 2 * pair + half, :8, half] = 0.5 * weight * np.cos(phi)
            inverse_cols[pair, 2 * pair + half, 8:, half] = -0.5 * weight * np.sin(phi)
    return (
        forward_rows,
        forward_cols,
        inverse_rows.reshape(128, 512),
        inverse_cols.reshape(4 * 128, 256),
    )


def halves_of_table(table):
    table = jnp.asarray(table.astype(np.float32))
    high = table.astype(BF16)
    low = (table - high.astype(F32)).astype(BF16)
    return high, low


def split(value):
    high = value.astype(BF16)
    return high, (value - high.astype(F32)).astype(BF16)


def matmul(left, right):
    return jnp.dot(left, right, preferred_element_type=F32)


def product(left, right):
    left_high, left_low = left
    right_high, right_low = right
    return (
        matmul(left_high, right_high) + matmul(left_high, right_low) + matmul(left_low, right_high)
    )


def gelu_of_double(half):
    inner = half * (2.0 * GELU_SCALE + (8.0 * GELU_SCALE * 0.044715) * (half * half))
    return half + half * jnp.tanh(inner)


def pooled_blocks(flat):
    pool_columns, pool_rows = pool_tables()
    high, low = split(flat)
    across = matmul(jnp.concatenate([high, low], axis=1), pool_columns)
    high, low = split(across)
    pooled = matmul(pool_rows, jnp.concatenate([high, low], axis=0))
    lane = lax.broadcasted_iota(jnp.int32, (8, 128), 1)
    first = lane < LANE_L3
    second = (lane >= LANE_L2) & (lane < LANE_L3_COPY)
    upper = []
    lower = []
    for channel in range(3):
        base = channel * 32
        coarse = jnp.where(second, pooled[base + 16 : base + 24], pooled[base + 24 : base + 32])
        upper.append(jnp.where(first, pooled[base : base + 8], coarse))
        lower.append(jnp.where(first, pooled[base + 8 : base + 16], coarse))
    return upper, lower


def emit_slots(slots_ref, position, upper, lower):
    count = slots_ref.shape[0]
    for slot in range(count):
        ahead = lax.rem(slot - position + count, count) < count // 2
        for channel in range(3):
            slots_ref[slot, channel] = jnp.where(ahead, lower[channel], upper[channel])


def near_tiles(pieces, kept):
    lane = lax.broadcasted_iota(jnp.int32, (8, 128), 1)
    shared = jnp.where(
        kept, pltpu.roll(pieces[0], 112, 1), pltpu.roll(pltpu.roll(pieces[1], 112, 1), 4, 0)
    )
    rest = jnp.where(lane < 96, shared, pltpu.roll(pieces[2], 16, 1))
    return (
        jnp.where(lane < 64, pieces[0], pltpu.roll(pieces[1], 64, 1)),
        jnp.where(lane < 64, pieces[2], rest),
    )


def far_tiles(pieces):
    lane = lax.broadcasted_iota(jnp.int32, (8, 128), 1)
    return (
        jnp.where(lane < 64, pltpu.roll(pieces[0], 64, 1), pieces[1]),
        pltpu.roll(pieces[2], 64, 1),
    )


def emit_row_slots(slots_ref, position, upper, lower):
    top = lax.broadcasted_iota(jnp.int32, (8, 128), 0) < 4
    near = near_tiles(upper, top), near_tiles(lower, jnp.logical_not(top))
    far = far_tiles(upper), far_tiles(lower)
    count = slots_ref.shape[0]
    for slot in range(count):
        distance = lax.rem(slot - position + count, count)
        ahead = distance < count // 2
        beside = (distance == 1) | (distance == count - 1)
        for tile in range(2):
            slots_ref[slot, tile] = jnp.where(
                beside,
                jnp.where(ahead, near[1][tile], near[0][tile]),
                jnp.where(ahead, far[1][tile], far[0][tile]),
            )


def received_rows(got_ref, position, columns, rows):
    lane = lax.broadcasted_iota(jnp.int32, (8, 128), 1)
    first = lane < LANE_L3
    second = (lane >= LANE_L2) & (lane < LANE_L3_COPY)
    near = {}
    for offset in (-4, -3, -2, 2, 3, 4):
        place = lax.rem(position + offset + 16, 16)
        head, tail = got_ref[place, 0], got_ref[place, 1]
        near[offset] = [pltpu.roll(head, 64, 1), head, pltpu.roll(tail, 64, 1)]
    beside = []
    for offset in (-1, 1):
        place = lax.rem(position + offset + 16, 16)
        head, tail = got_ref[place, 0], got_ref[place, 1]
        beside.append(jnp.where(first, head, tail))
        beside.append(jnp.where(first, pltpu.roll(head, 64, 1), pltpu.roll(tail, 4, 0)))
        beside.append(jnp.where(first, tail, pltpu.roll(tail, 96, 1)))
    high, low = split(jnp.concatenate(beside, axis=0))
    across = matmul(jnp.concatenate([high, low], axis=1), columns)
    high, low = split(jnp.concatenate([across[:, :128], across[:, 128:]], axis=0))
    pooled = matmul(rows, jnp.concatenate([high, low], axis=0))
    for side, offset in enumerate((-1, 1)):
        near[offset] = []
        for channel in range(3):
            base = side * 24 + channel * 8
            coarse = jnp.where(
                second, pooled[base : base + 8], pooled[48 + base : 48 + base + 8]
            )
            near[offset].append(jnp.where(first, beside[side * 3 + channel], coarse))
    return near


def pool_kernel(current_ref, slots_ref, own_ref):
    flat = current_ref[...].reshape(96, 128)
    upper, lower = pooled_blocks(flat)
    for channel in range(3):
        own_ref[0, channel] = upper[channel]
        own_ref[1, channel] = lower[channel]
    emit_row_slots(slots_ref, lax.axis_index("gx"), upper, lower)


def strip_kernel(own_ref, got_ref, columns_ref, rows_ref, ready_ref, slots_ref, strip_ref):
    received = received_rows(got_ref, lax.axis_index("gx"), columns_ref[...], rows_ref[...])
    lane = lax.broadcasted_iota(jnp.int32, (8, 128), 1)
    sub = lax.broadcasted_iota(jnp.int32, (8, 128), 0)
    first = lane < LANE_L3
    second = (lane >= LANE_L2) & (lane < LANE_L3_COPY)
    top = sub < 4
    low_two = sub < 2
    high_two = sub >= 6
    quarter = lane // 32

    upper_out = []
    lower_out = []
    for channel in range(3):
        near = {offset: blocks[channel] for offset, blocks in received.items()}
        near[0] = own_ref[0, channel]
        finest = [near[-1], own_ref[0, channel], own_ref[1, channel], near[1]]
        middle = [(-2, -1), (-1, 0), (0, 1), (1, 2)]
        coarse = [(-4, -3, -2), (-2, -1, 0), (0, 1, 2), (2, 3, 4)]
        upper = jnp.zeros((8, 128), F32)
        lower = jnp.zeros((8, 128), F32)
        for block in range(4):
            before, after = middle[block]
            start, centre, end = coarse[block]
            wide = jnp.where(
                low_two, near[start], jnp.where(high_two, near[end], near[centre])
            )
            value = jnp.where(
                first,
                finest[block],
                jnp.where(second, jnp.where(top, near[before], near[after]), wide),
            )
            strip_ref[channel, block * 8 : block * 8 + 8] = value
            here = quarter == block
            upper = jnp.where(here, pltpu.roll(value, (32 * block - 64) % 128, 1), upper)
            lower = jnp.where(here, pltpu.roll(value, (32 * block - 96) % 128, 1), lower)
        upper_out.append(upper)
        lower_out.append(lower)
    emit_slots(slots_ref, lax.axis_index("gy"), upper_out, lower_out)


def stacked_left(value):
    high, low = split(value)
    return jnp.concatenate([high, high, low], axis=1)


def stacked_right(value):
    high, low = split(value)
    return jnp.concatenate([high, low, high], axis=0)


def prepare_kernel(
    lift_ref,
    lift_bias_ref,
    weight_ref,
    bypass_ref,
    layer_bias_ref,
    mlp_in_ref,
    mlp_in_bias_ref,
    mlp_out_ref,
    mlp_out_bias_ref,
    project_ref,
    project_bias_ref,
    mixing_ref,
    skip_ref,
    inner_ref,
    inner_bias_ref,
    last_ref,
    offset_ref,
):
    highest = lax.Precision.HIGHEST
    lift = jnp.concatenate(
        [lift_ref[...], lift_bias_ref[...], jnp.zeros((PADDED - FEATURES - 1, 64), F32)], axis=0
    )
    left = stacked_left(lift)

    def mode_step(mode, carry):
        both = jnp.concatenate([weight_ref[0, mode], weight_ref[1, mode]], axis=1)
        mixing_ref[pl.ds(mode, PADDED, stride=64), :] = matmul(left, stacked_right(both))
        return carry

    lax.fori_loop(0, 64, mode_step, 0, unroll=8)

    skip = jnp.dot(lift, bypass_ref[...], precision=highest)
    row = lax.broadcasted_iota(jnp.int32, skip.shape, 0)
    skip = skip + jnp.where(row == FEATURES, layer_bias_ref[...], 0.0)
    square = jnp.concatenate([0.5 * skip, jnp.zeros((128 - PADDED, 64), F32)], axis=0)
    square = jnp.concatenate([square, jnp.zeros((128, 64), F32)], axis=1)
    skip_ref[...] = stacked_left(jnp.transpose(square)[:64, :PADDED])

    project = jnp.concatenate([project_ref[...], jnp.zeros((5, 64), F32)], axis=0)
    wide = jnp.concatenate([mlp_in_ref[...], jnp.zeros((64, 128), F32)], axis=0)
    inner = jnp.concatenate([0.5 * jnp.transpose(wide)[:, :64], project], axis=0)
    inner_ref[...] = stacked_left(inner)
    inner_bias_ref[...] = jnp.transpose(
        jnp.broadcast_to(0.5 * mlp_in_bias_ref[...], (128, 128))
    )
    last = jnp.dot(project, mlp_out_ref[...], precision=highest)
    for channel in range(3):
        last_ref[channel] = jnp.transpose(
            jnp.broadcast_to(last[channel : channel + 1], (128, 128))
        )
    sub = lax.broadcasted_iota(jnp.int32, (8, 3), 0)
    lane = lax.broadcasted_iota(jnp.int32, (8, 3), 1)
    constant = jnp.sum(project * mlp_out_bias_ref[...], axis=1, keepdims=True) + jnp.sum(
        jnp.where(sub == lane, project_bias_ref[...], 0.0), axis=1, keepdims=True
    )
    offset_ref[...] = jnp.broadcast_to(constant, (8, 128))


def contexts(strip_ref, twin_ref, other_ref, got_ref, position, channel, block):
    lane = lax.broadcasted_iota(jnp.int32, (8, 128), 1)
    rows = slice(block * 8, block * 8 + 8)
    here = strip_ref[channel, rows]
    twin = twin_ref[channel, rows]
    other = other_ref[channel, rows]
    even = position % 2 == 0
    before = jnp.where(even, other, twin)
    after = jnp.where(even, twin, other)
    far = {
        offset: got_ref[lax.rem(position + offset + 32, 32), channel]
        for offset in (-4, -3, -2, 2, 3, 4)
    }
    packed = 32 * block

    def moved(value, source, target):
        shift = (target - source) % 128
        return value if shift == 0 else pltpu.roll(value, shift, 1)

    def gathered(pieces):
        result = moved(*pieces[-1][1:])
        for piece in reversed(pieces[:-1]):
            result = jnp.where(lane < piece[0], moved(*piece[1:]), result)
        return result

    first = gathered([(32, before, 32, 0), (96, here, 0, 32), (128, after, 0, 96)])
    second = gathered(
        [
            (16, far[-2], packed, 0),
            (48, before, LANE_L2, 16),
            (80, here, LANE_L2, 48),
            (112, after, LANE_L2, 80),
            (128, far[2], packed + 16, 112),
        ]
    )
    third = gathered(
        [
            (8, far[-4], packed + 24, 0),
            (24, far[-3], packed + 16, 8),
            (40, far[-2], packed + 16, 24),
            (56, before, LANE_L3, 40),
            (72, here, LANE_L3, 56),
            (88, after, LANE_L3, 72),
            (104, far[2], packed, 88),
            (120, far[3], packed, 104),
            (128, far[4], packed, 120),
        ]
    )
    return first, second, third


def tile_step(
    current_ref,
    strip_ref,
    twin_ref,
    other_ref,
    got_ref,
    mixing_ref,
    skip_ref,
    inner_ref,
    inner_bias_ref,
    last_ref,
    offset_ref,
    rows_high_ref,
    rows_low_ref,
    cols_high_ref,
    cols_low_ref,
    back_rows_high_ref,
    back_rows_low_ref,
    back_cols_high_ref,
    back_cols_low_ref,
    features_ref,
    results_ref,
    partial_ref,
):
    position = lax.axis_index("gy")
    for channel in range(3):
        for block in range(4):
            pieces = (
                current_ref[channel, block * 8 : block * 8 + 8],
                *contexts(strip_ref, twin_ref, other_ref, got_ref, position, channel, block),
            )
            for level in range(4):
                features_ref[
                    pl.ds(block * 8 * PADDED + level * 3 + channel, 8, stride=PADDED), :
                ] = pieces[level]
    for row in range(ROWS):
        tail = lax.broadcasted_iota(jnp.int32, (4, 128), 0)
        features_ref[row * PADDED + FEATURES : (row + 1) * PADDED, :] = jnp.where(
            tail == 0, 1.0, 0.0
        )

    features = split(features_ref[...])
    along_rows = product((rows_high_ref[...], rows_low_ref[...]), features)
    contract = (((1,), (1,)), ((), ()))
    along_high, along_low = split(along_rows)

    def transposed(left, right):
        return lax.dot_general(left, right, contract, preferred_element_type=F32)

    spectrum = (
        transposed(cols_high_ref[...], along_high)
        + transposed(cols_high_ref[...], along_low)
        + transposed(cols_low_ref[...], along_high)
    )
    real = spectrum[:8, :128] - spectrum[8:, 128:]
    imag = spectrum[8:, :128] + spectrum[:8, 128:]
    lane = lax.broadcasted_iota(jnp.int32, (8, 128), 1)
    sub = lax.broadcasted_iota(jnp.int32, (8, 128), 0)
    real = jnp.where(
        (lane == 8 * FEATURES) & (sub == 0), float(ROWS * COLS), jnp.where(lane < 96, real, 0.0)
    )
    modes = []
    sign = jnp.where(lane < 64, -1.0, 1.0)
    for mode in range(8):
        with_real = None
        with_imag = None
        for feature in range(FEATURES + (1 if mode == 0 else 0)):
            place = feature * 8 + mode
            weights = mixing_ref[feature * 64 + mode * 8 : feature * 64 + mode * 8 + 8, :]
            term = jnp.broadcast_to(real[:, place : place + 1], (8, 128)) * weights
            with_real = term if with_real is None else with_real + term
            if feature < FEATURES:
                term = jnp.broadcast_to(imag[:, place : place + 1], (8, 128)) * weights
                with_imag = term if with_imag is None else with_imag + term
        modes.append(with_real + sign * pltpu.roll(with_imag, 64, 1))
    turned = jnp.transpose(jnp.concatenate(modes, axis=0))
    outputs = split(jnp.concatenate([turned[:64], turned[64:]], axis=1))
    back = product(outputs, (back_rows_high_ref[...], back_rows_low_ref[...]))
    stacked = split(
        jnp.concatenate([back[:, 128 * block : 128 * block + 128] for block in range(4)], axis=0)
    )

    skip = skip_ref[...]
    inner_left = inner_ref[...]
    inner_bias = jnp.concatenate([inner_bias_ref[...], inner_bias_ref[...]], axis=1)
    offset = jnp.concatenate([offset_ref[...], offset_ref[...]], axis=1)
    for pair in range(4):
        table = (
            back_cols_high_ref[pair * 128 : pair * 128 + 128, :],
            back_cols_low_ref[pair * 128 : pair * 128 + 128, :],
        )
        spectral = product(stacked, table)
        for block in range(4):
            row = block * 8 + pair * 2
            cells = jnp.concatenate(
                [
                    features_ref[row * PADDED : (row + 1) * PADDED, :],
                    features_ref[(row + 1) * PADDED : (row + 2) * PADDED, :],
                ],
                axis=1,
            )
            mixed = gelu_of_double(
                spectral[block * 64 : block * 64 + 64] + matmul(skip, stacked_right(cells))
            )
            wide = matmul(inner_left, stacked_right(mixed))
            hidden = gelu_of_double(wide[:128] + inner_bias)
            total = wide[128:136] + offset
            for half in range(2):
                lanes = slice(half * 128, half * 128 + 128)
                results_ref[(row + half) * 8 : (row + half) * 8 + 8, :] = total[:, lanes]
                for channel in range(3):
                    partial = None
                    for start in range(0, 128, 8):
                        term = hidden[start : start + 8, lanes] * last_ref[
                            channel, start : start + 8
                        ]
                        partial = term if partial is None else partial + term
                    partial_ref[channel, (row + half) * 8 : (row + half) * 8 + 8] = partial

    def sublane_sum(channel):
        total = results_ref[pl.ds(channel, ROWS, stride=8), :]
        for sub in range(8):
            total = total + partial_ref[channel, pl.ds(sub, ROWS, stride=8), :]
        return total

    return [current_ref[channel] + sublane_sum(channel) for channel in range(3)]


def final_kernel(*refs):
    next_ref = refs[19]
    updated = tile_step(*refs[:19], *refs[20:])
    for channel in range(3):
        next_ref[channel] = updated[channel]


def middle_kernel(*refs):
    next_ref, slots_ref, own_ref = refs[19:22]
    updated = tile_step(*refs[:19], *refs[22:])
    for channel in range(3):
        next_ref[channel] = updated[channel]
    upper, lower = pooled_blocks(jnp.concatenate(updated, axis=0))
    for channel in range(3):
        own_ref[0, channel] = upper[channel]
        own_ref[1, channel] = lower[channel]
    emit_row_slots(slots_ref, lax.axis_index("gx"), upper, lower)


VMEM = pl.BlockSpec(memory_space=pltpu.VMEM)


def resident(operand):
    return pltpu.with_memory_space_constraint(operand, pltpu.VMEM)


def call(body, name, operands, results, scratch=()):
    return pl.pallas_call(
        body,
        name=name,
        out_shape=[pltpu.VMEM(*(r if isinstance(r[0], tuple) else (r, F32))) for r in results],
        in_specs=[VMEM] * len(operands),
        out_specs=[VMEM] * len(results),
        scratch_shapes=list(scratch),
        compiler_params=pltpu.CompilerParams(vmem_limit_bytes=16 << 20),
    )(
        *(
            operand if operand.ndim == 4 and operand.shape[1] == 64 else resident(operand)
            for operand in operands
        )
    )


def shards(
    fields,
    lift_weight,
    lift_bias,
    spectral_weight,
    bypass_weight,
    layer_bias,
    mlp_in_weight,
    mlp_in_bias,
    mlp_out_weight,
    mlp_out_bias,
    project_weight,
    project_bias,
):
    n_gx = lax.axis_size("gx")
    n_gy = lax.axis_size("gy")
    tables = [half for table in fourier_tables() for half in halves_of_table(table)]

    refill = [jnp.asarray(table).astype(BF16) for table in refill_tables()]

    block = (3, 8, 128)
    row_block = (2, 8, 128)
    slots_x, own = call(
        pool_kernel, "pool", [fields], [(n_gx, *row_block), (2, *block)]
    )
    prepared = call(
        prepare_kernel,
        "prepare",
        [
            lift_weight,
            lift_bias[None],
            spectral_weight.reshape(2, 64, 64, 64),
            bypass_weight,
            layer_bias[None],
            mlp_in_weight,
            mlp_in_bias[None],
            mlp_out_weight.T,
            mlp_out_bias[None],
            project_weight.T,
            project_bias[None],
        ],
        [
            (PADDED * 64, 128),
            ((64, 3 * PADDED), BF16),
            ((136, 192), BF16),
            (128, 128),
            (3, 128, 128),
            (8, 128),
        ],
    )

    twins = [(i, i ^ 1) for i in range(n_gy)]
    others = [(i, (i + 1 if i % 2 else i - 1) % n_gy) for i in range(n_gy)]
    current = fields
    for step in range(STEPS):
        got_x = lax.all_to_all(slots_x, "gx", 0, 0, tiled=True)
        slots_y, strip = call(
            strip_kernel, "strip", [own, got_x, *refill, prepared[-1]], [(n_gy, *block), (3, ROWS, 128)]
        )
        got_y = lax.all_to_all(slots_y, "gy", 0, 0, tiled=True)
        twin = lax.ppermute(strip, "gy", twins)
        other = lax.ppermute(strip, "gy", others)
        operands = [
            current,
            strip,
            twin,
            other,
            got_y,
            *prepared,
            *tables,
        ]
        scratch = [pltpu.VMEM((ROWS * PADDED, 128), F32), pltpu.VMEM((ROWS * 8, 128), F32), pltpu.VMEM((3, ROWS * 8, 128), F32)]
        if step + 1 < STEPS:
            current, slots_x, own = call(
                middle_kernel,
                "middle",
                operands,
                [fields.shape, (n_gx, *row_block), (2, *block)],
                scratch,
            )
        else:
            (current,) = call(final_kernel, "final", operands, [fields.shape], scratch)
    return current


def solution(mesh):
    placed = (P(None, "gx", "gy"), P(), P(), P(), P(), P(), P(), P(), P(), P(), P(), P())
    return jax.shard_map(
        shards, mesh=mesh, in_specs=placed, out_specs=P(None, "gx", "gy"), check_vma=False
    )
```

```python
import math

import jax
import jax.numpy as jnp
import numpy as np
from jax import lax
from jax.experimental import pallas as pl
from jax.experimental.pallas import tpu as pltpu
from jax.sharding import PartitionSpec as P

STEPS = 2
ROWS = 32
COLS = 128
FEATURES = 12
PADDED = 16
LANE_L3 = 64
LANE_L2 = 80
LANE_L3_COPY = 112

BF16 = jnp.bfloat16
F32 = jnp.float32
GELU_SCALE = math.sqrt(2.0 / math.pi)


def refill_tables():
    columns = np.zeros((128, 256), np.float32)
    for cell in range(64):
        columns[cell, LANE_L2 + cell // 2] = 0.5
        columns[cell, LANE_L3 + cell // 4] = 0.25
        columns[cell, LANE_L3_COPY + cell // 4] = 0.25
    for cell in range(32):
        columns[64 + cell, 128 + LANE_L2 + cell] = 1.0
        columns[64 + cell, 128 + LANE_L3 + cell // 2] = 0.5
        columns[64 + cell, 128 + LANE_L3_COPY + cell // 2] = 0.5
    rows = np.zeros((96, 96), np.float32)
    for side in range(2):
        for channel in range(3):
            base = side * 24 + channel * 8
            for sub in range(8):
                row = (sub + 4) % 8
                if (row >= 4) == (side == 0):
                    start = base + 2 * (row % 4)
                    rows[base + sub, start : start + 2] = 0.5
                else:
                    rows[base + sub, 48 + base + sub] = 1.0
                row = (sub + 2) % 4
                if (row >= 2) == (side == 0):
                    start = base + 4 * (row % 2)
                    rows[48 + base + sub, start : start + 4] = 0.25
                else:
                    start = 48 + base + (2 * row + 4) % 8
                    rows[48 + base + sub, start : start + 2] = 0.5
    return np.concatenate([columns, columns], axis=0), np.concatenate([rows, rows], axis=1)


def pool_tables():
    cell = lax.broadcasted_iota(jnp.int32, (COLS, 128), 0)
    lane = lax.broadcasted_iota(jnp.int32, (COLS, 128), 1)
    eighth = cell >> 3
    columns = jnp.where(
        lane < LANE_L3,
        jnp.where(cell >> 1 == lane, 0.5, 0.0),
        jnp.where(
            (lane >= LANE_L2) & (lane < LANE_L3_COPY),
            jnp.where(cell >> 2 == lane - LANE_L2, 0.25, 0.0),
            jnp.where(
                (eighth == lane - LANE_L3) | (eighth == lane - LANE_L3_COPY), 0.125, 0.0
            ),
        ),
    ).astype(BF16)
    out = lax.broadcasted_iota(jnp.int32, (96, 96), 0)
    cell = lax.broadcasted_iota(jnp.int32, (96, 96), 1)
    kind = (out >> 3) & 3
    sub = out & 7
    row = cell & 31
    fine = jnp.where(row >> 1 == sub + 8 * kind, 0.5, 0.0)
    middle = jnp.where(row >> 2 == ((sub + 4) & 7), 0.25, 0.0)
    coarse = jnp.where(row >> 3 == ((sub + 2) & 3), 0.125, 0.0)
    rows = jnp.where(kind < 2, fine, jnp.where(kind == 2, middle, coarse))
    rows = jnp.where(out >> 5 == cell >> 5, rows, 0.0).astype(BF16)
    return jnp.concatenate([columns, columns], axis=0), jnp.concatenate([rows, rows], axis=1)


def fourier_tables():
    signed = np.array([0, 1, 2, 3, -4, -3, -2, -1])
    theta = 2.0 * np.pi * ((signed[:, None] * np.arange(ROWS)[None, :]) % ROWS) / ROWS
    phi = 2.0 * np.pi * ((np.arange(8)[:, None] * np.arange(COLS)[None, :]) % COLS) / COLS
    forward_rows = np.zeros((256, ROWS * PADDED))
    for feature in range(FEATURES):
        for mode in range(8):
            for row in range(ROWS):
                forward_rows[feature * 8 + mode, row * PADDED + feature] = math.cos(
                    theta[mode, row]
                )
                forward_rows[128 + feature * 8 + mode, row * PADDED + feature] = -math.sin(
                    theta[mode, row]
                )
    forward_cols = np.concatenate([np.cos(phi), -np.sin(phi)], axis=0)
    inverse_rows = np.zeros((2, 8, 8, ROWS, 2, 8))
    for mode in range(8):
        for column in range(8):
            inverse_rows[0, mode, column, :, 0, column] = np.cos(theta[mode])
            inverse_rows[1, mode, column, :, 0, column] = -np.sin(theta[mode])
            inverse_rows[0, mode, column, :, 1, column] = np.sin(theta[mode])
            inverse_rows[1, mode, column, :, 1, column] = np.cos(theta[mode])
    weight = np.where(np.arange(8) == 0, 1.0, 2.0)[:, None] / (ROWS * COLS)
    inverse_cols = np.zeros((4, 8, 16, 2, COLS))
    for pair in range(4):
        for half in range(2):
            inverse_cols[pair, 2 * pair + half, :8, half] = 0.5 * weight * np.cos(phi)
            inverse_cols[pair, 2 * pair + half, 8:, half] = -0.5 * weight * np.sin(phi)
    return (
        forward_rows,
        forward_cols,
        inverse_rows.reshape(128, 512),
        inverse_cols.reshape(4 * 128, 256),
    )


def halves_of_table(table):
    table = jnp.asarray(table.astype(np.float32))
    high = table.astype(BF16)
    low = (table - high.astype(F32)).astype(BF16)
    return high, low


def split(value):
    high = value.astype(BF16)
    return high, (value - high.astype(F32)).astype(BF16)


def matmul(left, right):
    return jnp.dot(left, right, preferred_element_type=F32)


def product(left, right):
    left_high, left_low = left
    right_high, right_low = right
    return (
        matmul(left_high, right_high) + matmul(left_high, right_low) + matmul(left_low, right_high)
    )


def gelu_of_double(half):
    inner = half * (2.0 * GELU_SCALE + (8.0 * GELU_SCALE * 0.044715) * (half * half))
    return half + half * jnp.tanh(inner)


def pooled_blocks(flat):
    pool_columns, pool_rows = pool_tables()
    high, low = split(flat)
    across = matmul(jnp.concatenate([high, low], axis=1), pool_columns)
    high, low = split(across)
    pooled = matmul(pool_rows, jnp.concatenate([high, low], axis=0))
    lane = lax.broadcasted_iota(jnp.int32, (8, 128), 1)
    first = lane < LANE_L3
    second = (lane >= LANE_L2) & (lane < LANE_L3_COPY)
    upper = []
    lower = []
    for channel in range(3):
        base = channel * 32
        coarse = jnp.where(second, pooled[base + 16 : base + 24], pooled[base + 24 : base + 32])
        upper.append(jnp.where(first, pooled[base : base + 8], coarse))
        lower.append(jnp.where(first, pooled[base + 8 : base + 16], coarse))
    return upper, lower


def emit_slots(slots_ref, position, upper, lower):
    count = slots_ref.shape[0]
    for slot in range(count):
        ahead = lax.rem(slot - position + count, count) < count // 2
        for channel in range(3):
            slots_ref[slot, channel] = jnp.where(ahead, lower[channel], upper[channel])


def near_tiles(pieces, kept):
    lane = lax.broadcasted_iota(jnp.int32, (8, 128), 1)
    shared = jnp.where(
        kept, pltpu.roll(pieces[0], 112, 1), pltpu.roll(pltpu.roll(pieces[1], 112, 1), 4, 0)
    )
    rest = jnp.where(lane < 96, shared, pltpu.roll(pieces[2], 16, 1))
    return (
        jnp.where(lane < 64, pieces[0], pltpu.roll(pieces[1], 64, 1)),
        jnp.where(lane < 64, pieces[2], rest),
    )


def far_tiles(pieces):
    lane = lax.broadcasted_iota(jnp.int32, (8, 128), 1)
    return (
        jnp.where(lane < 64, pltpu.roll(pieces[0], 64, 1), pieces[1]),
        pltpu.roll(pieces[2], 64, 1),
    )


def emit_row_slots(slots_ref, position, upper, lower):
    top = lax.broadcasted_iota(jnp.int32, (8, 128), 0) < 4
    near = near_tiles(upper, top), near_tiles(lower, jnp.logical_not(top))
    far = far_tiles(upper), far_tiles(lower)
    count = slots_ref.shape[0]
    for slot in range(count):
        distance = lax.rem(slot - position + count, count)
        ahead = distance < count // 2
        beside = (distance == 1) | (distance == count - 1)
        for tile in range(2):
            slots_ref[slot, tile] = jnp.where(
                beside,
                jnp.where(ahead, near[1][tile], near[0][tile]),
                jnp.where(ahead, far[1][tile], far[0][tile]),
            )


def received_rows(got_ref, position, columns, rows):
    lane = lax.broadcasted_iota(jnp.int32, (8, 128), 1)
    first = lane < LANE_L3
    second = (lane >= LANE_L2) & (lane < LANE_L3_COPY)
    near = {}
    for offset in (-4, -3, -2, 2, 3, 4):
        place = lax.rem(position + offset + 16, 16)
        head, tail = got_ref[place, 0], got_ref[place, 1]
        near[offset] = [pltpu.roll(head, 64, 1), head, pltpu.roll(tail, 64, 1)]
    beside = []
    for offset in (-1, 1):
        place = lax.rem(position + offset + 16, 16)
        head, tail = got_ref[place, 0], got_ref[place, 1]
        beside.append(jnp.where(first, head, tail))
        beside.append(jnp.where(first, pltpu.roll(head, 64, 1), pltpu.roll(tail, 4, 0)))
        beside.append(jnp.where(first, tail, pltpu.roll(tail, 96, 1)))
    high, low = split(jnp.concatenate(beside, axis=0))
    across = matmul(jnp.concatenate([high, low], axis=1), columns)
    high, low = split(jnp.concatenate([across[:, :128], across[:, 128:]], axis=0))
    pooled = matmul(rows, jnp.concatenate([high, low], axis=0))
    for side, offset in enumerate((-1, 1)):
        near[offset] = []
        for channel in range(3):
            base = side * 24 + channel * 8
            coarse = jnp.where(
                second, pooled[base : base + 8], pooled[48 + base : 48 + base + 8]
            )
            near[offset].append(jnp.where(first, beside[side * 3 + channel], coarse))
    return near


def pool_kernel(current_ref, slots_ref, own_ref):
    flat = current_ref[...].reshape(96, 128)
    upper, lower = pooled_blocks(flat)
    for channel in range(3):
        own_ref[0, channel] = upper[channel]
        own_ref[1, channel] = lower[channel]
    emit_row_slots(slots_ref, lax.axis_index("gx"), upper, lower)


def strip_kernel(own_ref, got_ref, columns_ref, rows_ref, ready_ref, slots_ref, strip_ref):
    received = received_rows(got_ref, lax.axis_index("gx"), columns_ref[...], rows_ref[...])
    lane = lax.broadcasted_iota(jnp.int32, (8, 128), 1)
    sub = lax.broadcasted_iota(jnp.int32, (8, 128), 0)
    first = lane < LANE_L3
    second = (lane >= LANE_L2) & (lane < LANE_L3_COPY)
    top = sub < 4
    low_two = sub < 2
    high_two = sub >= 6
    quarter = lane // 32

    upper_out = []
    lower_out = []
    for channel in range(3):
        near = {offset: blocks[channel] for offset, blocks in received.items()}
        near[0] = own_ref[0, channel]
        finest = [near[-1], own_ref[0, channel], own_ref[1, channel], near[1]]
        middle = [(-2, -1), (-1, 0), (0, 1), (1, 2)]
        coarse = [(-4, -3, -2), (-2, -1, 0), (0, 1, 2), (2, 3, 4)]
        upper = jnp.zeros((8, 128), F32)
        lower = jnp.zeros((8, 128), F32)
        for block in range(4):
            before, after = middle[block]
            start, centre, end = coarse[block]
            wide = jnp.where(
                low_two, near[start], jnp.where(high_two, near[end], near[centre])
            )
            value = jnp.where(
                first,
                finest[block],
                jnp.where(second, jnp.where(top, near[before], near[after]), wide),
            )
            strip_ref[channel, block * 8 : block * 8 + 8] = value
            here = quarter == block
            upper = jnp.where(here, pltpu.roll(value, (32 * block - 64) % 128, 1), upper)
            lower = jnp.where(here, pltpu.roll(value, (32 * block - 96) % 128, 1), lower)
        upper_out.append(upper)
        lower_out.append(lower)
    emit_slots(slots_ref, lax.axis_index("gy"), upper_out, lower_out)


def stacked_left(value):
    high, low = split(value)
    return jnp.concatenate([high, high, low], axis=1)


def stacked_right(value):
    high, low = split(value)
    return jnp.concatenate([high, low, high], axis=0)


def prepare_kernel(
    lift_ref,
    lift_bias_ref,
    weight_ref,
    bypass_ref,
    layer_bias_ref,
    mlp_in_ref,
    mlp_in_bias_ref,
    mlp_out_ref,
    mlp_out_bias_ref,
    project_ref,
    project_bias_ref,
    mixing_ref,
    skip_ref,
    inner_ref,
    inner_bias_ref,
    last_ref,
    offset_ref,
):
    highest = lax.Precision.HIGHEST
    lift = jnp.concatenate(
        [lift_ref[...], lift_bias_ref[...], jnp.zeros((PADDED - FEATURES - 1, 64), F32)], axis=0
    )
    left = stacked_left(lift)

    def mode_step(mode, carry):
        both = jnp.concatenate([weight_ref[0, mode], weight_ref[1, mode]], axis=1)
        mixing_ref[pl.ds(mode, PADDED, stride=64), :] = matmul(left, stacked_right(both))
        return carry

    lax.fori_loop(0, 64, mode_step, 0, unroll=8)

    skip = jnp.dot(lift, bypass_ref[...], precision=highest)
    row = lax.broadcasted_iota(jnp.int32, skip.shape, 0)
    skip = skip + jnp.where(row == FEATURES, layer_bias_ref[...], 0.0)
    square = jnp.concatenate([0.5 * skip, jnp.zeros((128 - PADDED, 64), F32)], axis=0)
    square = jnp.concatenate([square, jnp.zeros((128, 64), F32)], axis=1)
    skip_ref[...] = stacked_left(jnp.transpose(square)[:64, :PADDED])

    project = jnp.concatenate([project_ref[...], jnp.zeros((5, 64), F32)], axis=0)
    wide = jnp.concatenate([mlp_in_ref[...], jnp.zeros((64, 128), F32)], axis=0)
    inner = jnp.concatenate([0.5 * jnp.transpose(wide)[:, :64], project], axis=0)
    inner_ref[...] = stacked_left(inner)
    inner_bias_ref[...] = jnp.transpose(
        jnp.broadcast_to(0.5 * mlp_in_bias_ref[...], (128, 128))
    )
    last = jnp.dot(project, mlp_out_ref[...], precision=highest)
    for channel in range(3):
        last_ref[channel] = jnp.transpose(
            jnp.broadcast_to(last[channel : channel + 1], (128, 128))
        )
    sub = lax.broadcasted_iota(jnp.int32, (8, 3), 0)
    lane = lax.broadcasted_iota(jnp.int32, (8, 3), 1)
    constant = jnp.sum(project * mlp_out_bias_ref[...], axis=1, keepdims=True) + jnp.sum(
        jnp.where(sub == lane, project_bias_ref[...], 0.0), axis=1, keepdims=True
    )
    offset_ref[...] = jnp.broadcast_to(constant, (8, 128))


def contexts(strip_ref, twin_ref, other_ref, got_ref, position, channel, block):
    lane = lax.broadcasted_iota(jnp.int32, (8, 128), 1)
    rows = slice(block * 8, block * 8 + 8)
    here = strip_ref[channel, rows]
    twin = twin_ref[channel, rows]
    other = other_ref[channel, rows]
    even = position % 2 == 0
    before = jnp.where(even, other, twin)
    after = jnp.where(even, twin, other)
    far = {
        offset: got_ref[lax.rem(position + offset + 32, 32), channel]
        for offset in (-4, -3, -2, 2, 3, 4)
    }
    packed = 32 * block

    def moved(value, source, target):
        shift = (target - source) % 128
        return value if shift == 0 else pltpu.roll(value, shift, 1)

    def gathered(pieces):
        result = moved(*pieces[-1][1:])
        for piece in reversed(pieces[:-1]):
            result = jnp.where(lane < piece[0], moved(*piece[1:]), result)
        return result

    first = gathered([(32, before, 32, 0), (96, here, 0, 32), (128, after, 0, 96)])
    second = gathered(
        [
            (16, far[-2], packed, 0),
            (48, before, LANE_L2, 16),
            (80, here, LANE_L2, 48),
            (112, after, LANE_L2, 80),
            (128, far[2], packed + 16, 112),
        ]
    )
    third = gathered(
        [
            (8, far[-4], packed + 24, 0),
            (24, far[-3], packed + 16, 8),
            (40, far[-2], packed + 16, 24),
            (56, before, LANE_L3, 40),
            (72, here, LANE_L3, 56),
            (88, after, LANE_L3, 72),
            (104, far[2], packed, 88),
            (120, far[3], packed, 104),
            (128, far[4], packed, 120),
        ]
    )
    return first, second, third


def tile_step(
    current_ref,
    strip_ref,
    twin_ref,
    other_ref,
    got_ref,
    mixing_ref,
    skip_ref,
    inner_ref,
    inner_bias_ref,
    last_ref,
    offset_ref,
    rows_high_ref,
    rows_low_ref,
    cols_high_ref,
    cols_low_ref,
    back_rows_high_ref,
    back_rows_low_ref,
    back_cols_high_ref,
    back_cols_low_ref,
    features_ref,
    results_ref,
    partial_ref,
):
    position = lax.axis_index("gy")
    for channel in range(3):
        for block in range(4):
            pieces = (
                current_ref[channel, block * 8 : block * 8 + 8],
                *contexts(strip_ref, twin_ref, other_ref, got_ref, position, channel, block),
            )
            for level in range(4):
                features_ref[
                    pl.ds(block * 8 * PADDED + level * 3 + channel, 8, stride=PADDED), :
                ] = pieces[level]
    for row in range(ROWS):
        tail = lax.broadcasted_iota(jnp.int32, (4, 128), 0)
        features_ref[row * PADDED + FEATURES : (row + 1) * PADDED, :] = jnp.where(
            tail == 0, 1.0, 0.0
        )

    features = split(features_ref[...])
    along_rows = product((rows_high_ref[...], rows_low_ref[...]), features)
    contract = (((1,), (1,)), ((), ()))
    along_high, along_low = split(along_rows)

    def transposed(left, right):
        return lax.dot_general(left, right, contract, preferred_element_type=F32)

    spectrum = (
        transposed(cols_high_ref[...], along_high)
        + transposed(cols_high_ref[...], along_low)
        + transposed(cols_low_ref[...], along_high)
    )
    real = spectrum[:8, :128] - spectrum[8:, 128:]
    imag = spectrum[8:, :128] + spectrum[:8, 128:]
    lane = lax.broadcasted_iota(jnp.int32, (8, 128), 1)
    sub = lax.broadcasted_iota(jnp.int32, (8, 128), 0)
    real = jnp.where(
        (lane == 8 * FEATURES) & (sub == 0), float(ROWS * COLS), jnp.where(lane < 96, real, 0.0)
    )
    modes = []
    sign = jnp.where(lane < 64, -1.0, 1.0)
    for mode in range(8):
        with_real = None
        with_imag = None
        for feature in range(FEATURES + (1 if mode == 0 else 0)):
            place = feature * 8 + mode
            weights = mixing_ref[feature * 64 + mode * 8 : feature * 64 + mode * 8 + 8, :]
            term = jnp.broadcast_to(real[:, place : place + 1], (8, 128)) * weights
            with_real = term if with_real is None else with_real + term
            if feature < FEATURES:
                term = jnp.broadcast_to(imag[:, place : place + 1], (8, 128)) * weights
                with_imag = term if with_imag is None else with_imag + term
        modes.append(with_real + sign * pltpu.roll(with_imag, 64, 1))
    turned = jnp.transpose(jnp.concatenate(modes, axis=0))
    outputs = split(jnp.concatenate([turned[:64], turned[64:]], axis=1))
    back = product(outputs, (back_rows_high_ref[...], back_rows_low_ref[...]))
    stacked = split(
        jnp.concatenate([back[:, 128 * block : 128 * block + 128] for block in range(4)], axis=0)
    )

    skip = skip_ref[...]
    inner_left = inner_ref[...]
    inner_bias = jnp.concatenate([inner_bias_ref[...], inner_bias_ref[...]], axis=1)
    offset = jnp.concatenate([offset_ref[...], offset_ref[...]], axis=1)
    for pair in range(4):
        table = (
            back_cols_high_ref[pair * 128 : pair * 128 + 128, :],
            back_cols_low_ref[pair * 128 : pair * 128 + 128, :],
        )
        spectral = product(stacked, table)
        for block in range(4):
            row = block * 8 + pair * 2
            cells = jnp.concatenate(
                [
                    features_ref[row * PADDED : (row + 1) * PADDED, :],
                    features_ref[(row + 1) * PADDED : (row + 2) * PADDED, :],
                ],
                axis=1,
            )
            mixed = gelu_of_double(
                spectral[block * 64 : block * 64 + 64] + matmul(skip, stacked_right(cells))
            )
            wide = matmul(inner_left, stacked_right(mixed))
            hidden = gelu_of_double(wide[:128] + inner_bias)
            total = wide[128:136] + offset
            for half in range(2):
                lanes = slice(half * 128, half * 128 + 128)
                results_ref[(row + half) * 8 : (row + half) * 8 + 8, :] = total[:, lanes]
                for channel in range(3):
                    partial = None
                    for start in range(0, 128, 8):
                        term = hidden[start : start + 8, lanes] * last_ref[
                            channel, start : start + 8
                        ]
                        partial = term if partial is None else partial + term
                    partial_ref[channel, (row + half) * 8 : (row + half) * 8 + 8] = partial

    def sublane_sum(channel):
        total = results_ref[pl.ds(channel, ROWS, stride=8), :]
        for sub in range(8):
            total = total + partial_ref[channel, pl.ds(sub, ROWS, stride=8), :]
        return total

    return [current_ref[channel] + sublane_sum(channel) for channel in range(3)]


def final_kernel(*refs):
    next_ref = refs[19]
    updated = tile_step(*refs[:19], *refs[20:])
    for channel in range(3):
        next_ref[channel] = updated[channel]


def middle_kernel(*refs):
    next_ref, slots_ref, own_ref = refs[19:22]
    updated = tile_step(*refs[:19], *refs[22:])
    for channel in range(3):
        next_ref[channel] = updated[channel]
    upper, lower = pooled_blocks(jnp.concatenate(updated, axis=0))
    for channel in range(3):
        own_ref[0, channel] = upper[channel]
        own_ref[1, channel] = lower[channel]
    emit_row_slots(slots_ref, lax.axis_index("gx"), upper, lower)


VMEM = pl.BlockSpec(memory_space=pltpu.VMEM)


def resident(operand):
    return pltpu.with_memory_space_constraint(operand, pltpu.VMEM)


def call(body, operands, results, scratch=()):
    return pl.pallas_call(
        body,
        out_shape=[pltpu.VMEM(*(r if isinstance(r[0], tuple) else (r, F32))) for r in results],
        in_specs=[VMEM] * len(operands),
        out_specs=[VMEM] * len(results),
        scratch_shapes=list(scratch),
        compiler_params=pltpu.CompilerParams(vmem_limit_bytes=16 << 20),
    )(
        *(
            operand if operand.ndim == 4 and operand.shape[1] == 64 else resident(operand)
            for operand in operands
        )
    )


def shards(
    fields,
    lift_weight,
    lift_bias,
    spectral_weight,
    bypass_weight,
    layer_bias,
    mlp_in_weight,
    mlp_in_bias,
    mlp_out_weight,
    mlp_out_bias,
    project_weight,
    project_bias,
):
    n_gx = lax.axis_size("gx")
    n_gy = lax.axis_size("gy")
    tables = [half for table in fourier_tables() for half in halves_of_table(table)]

    refill = [jnp.asarray(table).astype(BF16) for table in refill_tables()]

    block = (3, 8, 128)
    row_block = (2, 8, 128)
    slots_x, own = call(pool_kernel, [fields], [(n_gx, *row_block), (2, *block)])
    prepared = call(
        prepare_kernel,
        [
            lift_weight,
            lift_bias[None],
            spectral_weight.reshape(2, 64, 64, 64),
            bypass_weight,
            layer_bias[None],
            mlp_in_weight,
            mlp_in_bias[None],
            mlp_out_weight.T,
            mlp_out_bias[None],
            project_weight.T,
            project_bias[None],
        ],
        [
            (PADDED * 64, 128),
            ((64, 3 * PADDED), BF16),
            ((136, 192), BF16),
            (128, 128),
            (3, 128, 128),
            (8, 128),
        ],
    )

    twins = [(i, i ^ 1) for i in range(n_gy)]
    others = [(i, (i + 1 if i % 2 else i - 1) % n_gy) for i in range(n_gy)]
    current = fields
    for step in range(STEPS):
        got_x = lax.all_to_all(slots_x, "gx", 0, 0, tiled=True)
        slots_y, strip = call(
            strip_kernel, [own, got_x, *refill, prepared[-1]], [(n_gy, *block), (3, ROWS, 128)]
        )
        other = lax.ppermute(strip, "gy", others)
        got_y = lax.all_to_all(slots_y, "gy", 0, 0, tiled=True)
        twin = lax.ppermute(strip, "gy", twins)
        operands = [
            current,
            strip,
            twin,
            other,
            got_y,
            *prepared,
            *tables,
        ]
        scratch = [pltpu.VMEM((ROWS * PADDED, 128), F32), pltpu.VMEM((ROWS * 8, 128), F32), pltpu.VMEM((3, ROWS * 8, 128), F32)]
        if step + 1 < STEPS:
            current, slots_x, own = call(
                middle_kernel, operands, [fields.shape, (n_gx, *row_block), (2, *block)], scratch
            )
        else:
            (current,) = call(final_kernel, operands, [fields.shape], scratch)
    return current


def solution(mesh):
    placed = (P(None, "gx", "gy"), P(), P(), P(), P(), P(), P(), P(), P(), P(), P(), P())
    return jax.shard_map(
        shards, mesh=mesh, in_specs=placed, out_specs=P(None, "gx", "gy"), check_vma=False
    )
```

```python
import math

import jax
import jax.numpy as jnp
import numpy as np
from jax import lax
from jax.experimental import pallas as pl
from jax.experimental.pallas import tpu as pltpu
from jax.sharding import PartitionSpec as P

STEPS = 2
ROWS = 32
COLS = 128
FEATURES = 12
PADDED = 16
LANE_L3 = 64
LANE_L2 = 80
LANE_L3_COPY = 112

BF16 = jnp.bfloat16
F32 = jnp.float32
GELU_SCALE = math.sqrt(2.0 / math.pi)


def refill_tables():
    columns = np.zeros((128, 256), np.float32)
    for cell in range(64):
        columns[cell, LANE_L2 + cell // 2] = 0.5
        columns[cell, LANE_L3 + cell // 4] = 0.25
        columns[cell, LANE_L3_COPY + cell // 4] = 0.25
    for cell in range(32):
        columns[64 + cell, 128 + LANE_L2 + cell] = 1.0
        columns[64 + cell, 128 + LANE_L3 + cell // 2] = 0.5
        columns[64 + cell, 128 + LANE_L3_COPY + cell // 2] = 0.5
    rows = np.zeros((96, 96), np.float32)
    for side in range(2):
        for channel in range(3):
            base = side * 24 + channel * 8
            for sub in range(8):
                row = (sub + 4) % 8
                if (row >= 4) == (side == 0):
                    start = base + 2 * (row % 4)
                    rows[base + sub, start : start + 2] = 0.5
                else:
                    rows[base + sub, 48 + base + sub] = 1.0
                row = (sub + 2) % 4
                if (row >= 2) == (side == 0):
                    start = base + 4 * (row % 2)
                    rows[48 + base + sub, start : start + 4] = 0.25
                else:
                    start = 48 + base + (2 * row + 4) % 8
                    rows[48 + base + sub, start : start + 2] = 0.5
    return np.concatenate([columns, columns], axis=0), np.concatenate([rows, rows], axis=1)


def pool_tables():
    cell = lax.broadcasted_iota(jnp.int32, (COLS, 128), 0)
    lane = lax.broadcasted_iota(jnp.int32, (COLS, 128), 1)
    eighth = cell >> 3
    columns = jnp.where(
        lane < LANE_L3,
        jnp.where(cell >> 1 == lane, 0.5, 0.0),
        jnp.where(
            (lane >= LANE_L2) & (lane < LANE_L3_COPY),
            jnp.where(cell >> 2 == lane - LANE_L2, 0.25, 0.0),
            jnp.where(
                (eighth == lane - LANE_L3) | (eighth == lane - LANE_L3_COPY), 0.125, 0.0
            ),
        ),
    ).astype(BF16)
    out = lax.broadcasted_iota(jnp.int32, (96, 96), 0)
    cell = lax.broadcasted_iota(jnp.int32, (96, 96), 1)
    kind = (out >> 3) & 3
    sub = out & 7
    row = cell & 31
    fine = jnp.where(row >> 1 == sub + 8 * kind, 0.5, 0.0)
    middle = jnp.where(row >> 2 == ((sub + 4) & 7), 0.25, 0.0)
    coarse = jnp.where(row >> 3 == ((sub + 2) & 3), 0.125, 0.0)
    rows = jnp.where(kind < 2, fine, jnp.where(kind == 2, middle, coarse))
    rows = jnp.where(out >> 5 == cell >> 5, rows, 0.0).astype(BF16)
    return jnp.concatenate([columns, columns], axis=0), jnp.concatenate([rows, rows], axis=1)


def fourier_tables():
    signed = np.array([0, 1, 2, 3, -4, -3, -2, -1])
    theta = 2.0 * np.pi * ((signed[:, None] * np.arange(ROWS)[None, :]) % ROWS) / ROWS
    phi = 2.0 * np.pi * ((np.arange(8)[:, None] * np.arange(COLS)[None, :]) % COLS) / COLS
    forward_rows = np.zeros((256, ROWS * PADDED))
    for feature in range(FEATURES):
        for mode in range(8):
            for row in range(ROWS):
                forward_rows[feature * 8 + mode, row * PADDED + feature] = math.cos(
                    theta[mode, row]
                )
                forward_rows[128 + feature * 8 + mode, row * PADDED + feature] = -math.sin(
                    theta[mode, row]
                )
    forward_cols = np.concatenate([np.cos(phi), -np.sin(phi)], axis=0)
    inverse_rows = np.zeros((2, 8, 8, ROWS, 2, 8))
    for mode in range(8):
        for column in range(8):
            inverse_rows[0, mode, column, :, 0, column] = np.cos(theta[mode])
            inverse_rows[1, mode, column, :, 0, column] = -np.sin(theta[mode])
            inverse_rows[0, mode, column, :, 1, column] = np.sin(theta[mode])
            inverse_rows[1, mode, column, :, 1, column] = np.cos(theta[mode])
    weight = np.where(np.arange(8) == 0, 1.0, 2.0)[:, None] / (ROWS * COLS)
    inverse_cols = np.zeros((4, 8, 16, 2, COLS))
    for pair in range(4):
        for half in range(2):
            inverse_cols[pair, 2 * pair + half, :8, half] = 0.5 * weight * np.cos(phi)
            inverse_cols[pair, 2 * pair + half, 8:, half] = -0.5 * weight * np.sin(phi)
    return (
        forward_rows,
        forward_cols,
        inverse_rows.reshape(128, 512),
        inverse_cols.reshape(4 * 128, 256),
    )


def halves_of_table(table):
    table = jnp.asarray(table.astype(np.float32))
    high = table.astype(BF16)
    low = (table - high.astype(F32)).astype(BF16)
    return high, low


def split(value):
    high = value.astype(BF16)
    return high, (value - high.astype(F32)).astype(BF16)


def matmul(left, right):
    return jnp.dot(left, right, preferred_element_type=F32)


def product(left, right):
    left_high, left_low = left
    right_high, right_low = right
    return (
        matmul(left_high, right_high) + matmul(left_high, right_low) + matmul(left_low, right_high)
    )


def gelu_of_double(half):
    inner = half * (2.0 * GELU_SCALE + (8.0 * GELU_SCALE * 0.044715) * (half * half))
    return half + half * jnp.tanh(inner)


def pooled_blocks(flat):
    pool_columns, pool_rows = pool_tables()
    high, low = split(flat)
    across = matmul(jnp.concatenate([high, low], axis=1), pool_columns)
    high, low = split(across)
    pooled = matmul(pool_rows, jnp.concatenate([high, low], axis=0))
    lane = lax.broadcasted_iota(jnp.int32, (8, 128), 1)
    first = lane < LANE_L3
    second = (lane >= LANE_L2) & (lane < LANE_L3_COPY)
    upper = []
    lower = []
    for channel in range(3):
        base = channel * 32
        coarse = jnp.where(second, pooled[base + 16 : base + 24], pooled[base + 24 : base + 32])
        upper.append(jnp.where(first, pooled[base : base + 8], coarse))
        lower.append(jnp.where(first, pooled[base + 8 : base + 16], coarse))
    return upper, lower


def emit_slots(slots_ref, position, upper, lower):
    count = slots_ref.shape[0]
    for slot in range(count):
        ahead = lax.rem(slot - position + count, count) < count // 2
        for channel in range(3):
            slots_ref[slot, channel] = jnp.where(ahead, lower[channel], upper[channel])


def near_tiles(pieces, kept):
    lane = lax.broadcasted_iota(jnp.int32, (8, 128), 1)
    shared = jnp.where(
        kept, pltpu.roll(pieces[0], 112, 1), pltpu.roll(pltpu.roll(pieces[1], 112, 1), 4, 0)
    )
    rest = jnp.where(lane < 96, shared, pltpu.roll(pieces[2], 16, 1))
    return (
        jnp.where(lane < 64, pieces[0], pltpu.roll(pieces[1], 64, 1)),
        jnp.where(lane < 64, pieces[2], rest),
    )


def far_tiles(pieces):
    lane = lax.broadcasted_iota(jnp.int32, (8, 128), 1)
    return (
        jnp.where(lane < 64, pltpu.roll(pieces[0], 64, 1), pieces[1]),
        pltpu.roll(pieces[2], 64, 1),
    )


def emit_row_slots(slots_ref, position, upper, lower):
    top = lax.broadcasted_iota(jnp.int32, (8, 128), 0) < 4
    near = near_tiles(upper, top), near_tiles(lower, jnp.logical_not(top))
    far = far_tiles(upper), far_tiles(lower)
    count = slots_ref.shape[0]
    for slot in range(count):
        distance = lax.rem(slot - position + count, count)
        ahead = distance < count // 2
        beside = (distance == 1) | (distance == count - 1)
        for tile in range(2):
            slots_ref[slot, tile] = jnp.where(
                beside,
                jnp.where(ahead, near[1][tile], near[0][tile]),
                jnp.where(ahead, far[1][tile], far[0][tile]),
            )


def received_rows(got_ref, position, columns, rows):
    lane = lax.broadcasted_iota(jnp.int32, (8, 128), 1)
    first = lane < LANE_L3
    second = (lane >= LANE_L2) & (lane < LANE_L3_COPY)
    near = {}
    for offset in (-4, -3, -2, 2, 3, 4):
        place = lax.rem(position + offset + 16, 16)
        head, tail = got_ref[place, 0], got_ref[place, 1]
        near[offset] = [pltpu.roll(head, 64, 1), head, pltpu.roll(tail, 64, 1)]
    beside = []
    for offset in (-1, 1):
        place = lax.rem(position + offset + 16, 16)
        head, tail = got_ref[place, 0], got_ref[place, 1]
        beside.append(jnp.where(first, head, tail))
        beside.append(jnp.where(first, pltpu.roll(head, 64, 1), pltpu.roll(tail, 4, 0)))
        beside.append(jnp.where(first, tail, pltpu.roll(tail, 96, 1)))
    high, low = split(jnp.concatenate(beside, axis=0))
    across = matmul(jnp.concatenate([high, low], axis=1), columns)
    high, low = split(jnp.concatenate([across[:, :128], across[:, 128:]], axis=0))
    pooled = matmul(rows, jnp.concatenate([high, low], axis=0))
    for side, offset in enumerate((-1, 1)):
        near[offset] = []
        for channel in range(3):
            base = side * 24 + channel * 8
            coarse = jnp.where(
                second, pooled[base : base + 8], pooled[48 + base : 48 + base + 8]
            )
            near[offset].append(jnp.where(first, beside[side * 3 + channel], coarse))
    return near


def pool_kernel(current_ref, slots_ref, own_ref):
    flat = current_ref[...].reshape(96, 128)
    upper, lower = pooled_blocks(flat)
    for channel in range(3):
        own_ref[0, channel] = upper[channel]
        own_ref[1, channel] = lower[channel]
    emit_row_slots(slots_ref, lax.axis_index("gx"), upper, lower)


def strip_kernel(own_ref, got_ref, columns_ref, rows_ref, ready_ref, slots_ref, strip_ref):
    received = received_rows(got_ref, lax.axis_index("gx"), columns_ref[...], rows_ref[...])
    lane = lax.broadcasted_iota(jnp.int32, (8, 128), 1)
    sub = lax.broadcasted_iota(jnp.int32, (8, 128), 0)
    first = lane < LANE_L3
    second = (lane >= LANE_L2) & (lane < LANE_L3_COPY)
    top = sub < 4
    low_two = sub < 2
    high_two = sub >= 6
    quarter = lane // 32

    upper_out = []
    lower_out = []
    for channel in range(3):
        near = {offset: blocks[channel] for offset, blocks in received.items()}
        near[0] = own_ref[0, channel]
        finest = [near[-1], own_ref[0, channel], own_ref[1, channel], near[1]]
        middle = [(-2, -1), (-1, 0), (0, 1), (1, 2)]
        coarse = [(-4, -3, -2), (-2, -1, 0), (0, 1, 2), (2, 3, 4)]
        upper = jnp.zeros((8, 128), F32)
        lower = jnp.zeros((8, 128), F32)
        for block in range(4):
            before, after = middle[block]
            start, centre, end = coarse[block]
            wide = jnp.where(
                low_two, near[start], jnp.where(high_two, near[end], near[centre])
            )
            value = jnp.where(
                first,
                finest[block],
                jnp.where(second, jnp.where(top, near[before], near[after]), wide),
            )
            strip_ref[channel, block * 8 : block * 8 + 8] = value
            here = quarter == block
            upper = jnp.where(here, pltpu.roll(value, (32 * block - 64) % 128, 1), upper)
            lower = jnp.where(here, pltpu.roll(value, (32 * block - 96) % 128, 1), lower)
        upper_out.append(upper)
        lower_out.append(lower)
    emit_slots(slots_ref, lax.axis_index("gy"), upper_out, lower_out)


def stacked_left(value):
    high, low = split(value)
    return jnp.concatenate([high, high, low], axis=1)


def stacked_right(value):
    high, low = split(value)
    return jnp.concatenate([high, low, high], axis=0)


def prepare_kernel(
    lift_ref,
    lift_bias_ref,
    weight_ref,
    bypass_ref,
    layer_bias_ref,
    mlp_in_ref,
    mlp_in_bias_ref,
    mlp_out_ref,
    mlp_out_bias_ref,
    project_ref,
    project_bias_ref,
    mixing_ref,
    skip_ref,
    inner_ref,
    inner_bias_ref,
    last_ref,
    offset_ref,
):
    highest = lax.Precision.HIGHEST
    lift = jnp.concatenate(
        [lift_ref[...], lift_bias_ref[...], jnp.zeros((PADDED - FEATURES - 1, 64), F32)], axis=0
    )
    left = stacked_left(lift)

    def mode_step(mode, carry):
        both = jnp.concatenate([weight_ref[0, mode], weight_ref[1, mode]], axis=1)
        mixing_ref[pl.ds(mode, PADDED, stride=64), :] = matmul(left, stacked_right(both))
        return carry

    lax.fori_loop(0, 64, mode_step, 0, unroll=8)

    skip = jnp.dot(lift, bypass_ref[...], precision=highest)
    row = lax.broadcasted_iota(jnp.int32, skip.shape, 0)
    skip = skip + jnp.where(row == FEATURES, layer_bias_ref[...], 0.0)
    square = jnp.concatenate([0.5 * skip, jnp.zeros((128 - PADDED, 64), F32)], axis=0)
    square = jnp.concatenate([square, jnp.zeros((128, 64), F32)], axis=1)
    skip_ref[...] = stacked_left(jnp.transpose(square)[:64, :PADDED])

    project = jnp.concatenate([project_ref[...], jnp.zeros((5, 64), F32)], axis=0)
    wide = jnp.concatenate([mlp_in_ref[...], jnp.zeros((64, 128), F32)], axis=0)
    inner = jnp.concatenate([0.5 * jnp.transpose(wide)[:, :64], project], axis=0)
    inner_ref[...] = stacked_left(inner)
    inner_bias_ref[...] = jnp.transpose(
        jnp.broadcast_to(0.5 * mlp_in_bias_ref[...], (128, 128))
    )
    last = jnp.dot(project, mlp_out_ref[...], precision=highest)
    for channel in range(3):
        last_ref[channel] = jnp.transpose(
            jnp.broadcast_to(last[channel : channel + 1], (128, 128))
        )
    sub = lax.broadcasted_iota(jnp.int32, (8, 3), 0)
    lane = lax.broadcasted_iota(jnp.int32, (8, 3), 1)
    constant = jnp.sum(project * mlp_out_bias_ref[...], axis=1, keepdims=True) + jnp.sum(
        jnp.where(sub == lane, project_bias_ref[...], 0.0), axis=1, keepdims=True
    )
    offset_ref[...] = jnp.broadcast_to(constant, (8, 128))


def contexts(strip_ref, twin_ref, other_ref, got_ref, position, channel, block):
    lane = lax.broadcasted_iota(jnp.int32, (8, 128), 1)
    rows = slice(block * 8, block * 8 + 8)
    here = strip_ref[channel, rows]
    twin = twin_ref[channel, rows]
    other = other_ref[channel, rows]
    even = position % 2 == 0
    before = jnp.where(even, other, twin)
    after = jnp.where(even, twin, other)
    far = {
        offset: got_ref[lax.rem(position + offset + 32, 32), channel]
        for offset in (-4, -3, -2, 2, 3, 4)
    }
    packed = 32 * block

    def moved(value, source, target):
        shift = (target - source) % 128
        return value if shift == 0 else pltpu.roll(value, shift, 1)

    def gathered(pieces):
        result = moved(*pieces[-1][1:])
        for piece in reversed(pieces[:-1]):
            result = jnp.where(lane < piece[0], moved(*piece[1:]), result)
        return result

    first = gathered([(32, before, 32, 0), (96, here, 0, 32), (128, after, 0, 96)])
    second = gathered(
        [
            (16, far[-2], packed, 0),
            (48, before, LANE_L2, 16),
            (80, here, LANE_L2, 48),
            (112, after, LANE_L2, 80),
            (128, far[2], packed + 16, 112),
        ]
    )
    third = gathered(
        [
            (8, far[-4], packed + 24, 0),
            (24, far[-3], packed + 16, 8),
            (40, far[-2], packed + 16, 24),
            (56, before, LANE_L3, 40),
            (72, here, LANE_L3, 56),
            (88, after, LANE_L3, 72),
            (104, far[2], packed, 88),
            (120, far[3], packed, 104),
            (128, far[4], packed, 120),
        ]
    )
    return first, second, third


def tile_step(
    current_ref,
    strip_ref,
    twin_ref,
    other_ref,
    got_ref,
    mixing_ref,
    skip_ref,
    inner_ref,
    inner_bias_ref,
    last_ref,
    offset_ref,
    rows_high_ref,
    rows_low_ref,
    cols_high_ref,
    cols_low_ref,
    back_rows_high_ref,
    back_rows_low_ref,
    back_cols_high_ref,
    back_cols_low_ref,
    features_ref,
    results_ref,
    partial_ref,
):
    position = lax.axis_index("gy")
    for channel in range(3):
        for block in range(4):
            pieces = (
                current_ref[channel, block * 8 : block * 8 + 8],
                *contexts(strip_ref, twin_ref, other_ref, got_ref, position, channel, block),
            )
            for level in range(4):
                features_ref[
                    pl.ds(block * 8 * PADDED + level * 3 + channel, 8, stride=PADDED), :
                ] = pieces[level]
    for row in range(ROWS):
        tail = lax.broadcasted_iota(jnp.int32, (4, 128), 0)
        features_ref[row * PADDED + FEATURES : (row + 1) * PADDED, :] = jnp.where(
            tail == 0, 1.0, 0.0
        )

    features = split(features_ref[...])
    along_rows = product((rows_high_ref[...], rows_low_ref[...]), features)
    contract = (((1,), (1,)), ((), ()))
    along_high, along_low = split(along_rows)

    def transposed(left, right):
        return lax.dot_general(left, right, contract, preferred_element_type=F32)

    spectrum = (
        transposed(cols_high_ref[...], along_high)
        + transposed(cols_high_ref[...], along_low)
        + transposed(cols_low_ref[...], along_high)
    )
    real = spectrum[:8, :128] - spectrum[8:, 128:]
    imag = spectrum[8:, :128] + spectrum[:8, 128:]
    lane = lax.broadcasted_iota(jnp.int32, (8, 128), 1)
    sub = lax.broadcasted_iota(jnp.int32, (8, 128), 0)
    real = jnp.where(
        (lane == 8 * FEATURES) & (sub == 0), float(ROWS * COLS), jnp.where(lane < 96, real, 0.0)
    )
    modes = []
    sign = jnp.where(lane < 64, -1.0, 1.0)
    for mode in range(8):
        with_real = None
        with_imag = None
        for feature in range(FEATURES + (1 if mode == 0 else 0)):
            place = feature * 8 + mode
            weights = mixing_ref[feature * 64 + mode * 8 : feature * 64 + mode * 8 + 8, :]
            term = jnp.broadcast_to(real[:, place : place + 1], (8, 128)) * weights
            with_real = term if with_real is None else with_real + term
            if feature < FEATURES:
                term = jnp.broadcast_to(imag[:, place : place + 1], (8, 128)) * weights
                with_imag = term if with_imag is None else with_imag + term
        modes.append(with_real + sign * pltpu.roll(with_imag, 64, 1))
    turned = jnp.transpose(jnp.concatenate(modes, axis=0))
    outputs = split(jnp.concatenate([turned[:64], turned[64:]], axis=1))
    back = product(outputs, (back_rows_high_ref[...], back_rows_low_ref[...]))
    stacked = split(
        jnp.concatenate([back[:, 128 * block : 128 * block + 128] for block in range(4)], axis=0)
    )

    skip = skip_ref[...]
    inner_left = inner_ref[...]
    inner_bias = jnp.concatenate([inner_bias_ref[...], inner_bias_ref[...]], axis=1)
    offset = jnp.concatenate([offset_ref[...], offset_ref[...]], axis=1)
    pending = []

    def finish(row, mixed):
        wide = matmul(inner_left, stacked_right(mixed))
        hidden = gelu_of_double(wide[:128] + inner_bias)
        total = wide[128:136] + offset
        for half in range(2):
            lanes = slice(half * 128, half * 128 + 128)
            results_ref[(row + half) * 8 : (row + half) * 8 + 8, :] = total[:, lanes]
            for channel in range(3):
                partial_ref[channel, (row + half) * 8 : (row + half) * 8 + 8] = jnp.sum(
                    (hidden[:, lanes] * last_ref[channel]).reshape(16, 8, 128), axis=0
                )

    for pair in range(4):
        table = (
            back_cols_high_ref[pair * 128 : pair * 128 + 128, :],
            back_cols_low_ref[pair * 128 : pair * 128 + 128, :],
        )
        spectral = matmul(
            jnp.concatenate([stacked[0], stacked[0], stacked[1]], axis=1),
            jnp.concatenate([table[0], table[1], table[0]], axis=0),
        )
        for block in range(4):
            row = block * 8 + pair * 2
            high, low = (
                jnp.concatenate(
                    [
                        half[row * PADDED : (row + 1) * PADDED],
                        half[(row + 1) * PADDED : (row + 2) * PADDED],
                    ],
                    axis=1,
                )
                for half in features
            )
            cells = jnp.concatenate([high, low, high], axis=0)
            pending.append(
                (
                    row,
                    gelu_of_double(
                        spectral[block * 64 : block * 64 + 64] + matmul(skip, cells)
                    ),
                )
            )
            if len(pending) == 2:
                finish(*pending.pop(0))
    finish(*pending.pop(0))

    def sublane_sum(channel):
        total = results_ref[pl.ds(channel, ROWS, stride=8), :]
        for sub in range(8):
            total = total + partial_ref[channel, pl.ds(sub, ROWS, stride=8), :]
        return total

    return [current_ref[channel] + sublane_sum(channel) for channel in range(3)]


def final_kernel(*refs):
    next_ref = refs[19]
    updated = tile_step(*refs[:19], *refs[20:])
    for channel in range(3):
        next_ref[channel] = updated[channel]


def middle_kernel(*refs):
    next_ref, slots_ref, own_ref = refs[19:22]
    updated = tile_step(*refs[:19], *refs[22:])
    for channel in range(3):
        next_ref[channel] = updated[channel]
    upper, lower = pooled_blocks(jnp.concatenate(updated, axis=0))
    for channel in range(3):
        own_ref[0, channel] = upper[channel]
        own_ref[1, channel] = lower[channel]
    emit_row_slots(slots_ref, lax.axis_index("gx"), upper, lower)


VMEM = pl.BlockSpec(memory_space=pltpu.VMEM)


def resident(operand):
    return pltpu.with_memory_space_constraint(operand, pltpu.VMEM)


def call(body, name, operands, results, scratch=()):
    return pl.pallas_call(
        body,
        name=name,
        out_shape=[pltpu.VMEM(*(r if isinstance(r[0], tuple) else (r, F32))) for r in results],
        in_specs=[VMEM] * len(operands),
        out_specs=[VMEM] * len(results),
        scratch_shapes=list(scratch),
        compiler_params=pltpu.CompilerParams(vmem_limit_bytes=16 << 20),
    )(
        *(
            operand if operand.ndim == 4 and operand.shape[1] == 64 else resident(operand)
            for operand in operands
        )
    )


def shards(
    fields,
    lift_weight,
    lift_bias,
    spectral_weight,
    bypass_weight,
    layer_bias,
    mlp_in_weight,
    mlp_in_bias,
    mlp_out_weight,
    mlp_out_bias,
    project_weight,
    project_bias,
):
    n_gx = lax.axis_size("gx")
    n_gy = lax.axis_size("gy")
    tables = [half for table in fourier_tables() for half in halves_of_table(table)]

    refill = [jnp.asarray(table).astype(BF16) for table in refill_tables()]

    block = (3, 8, 128)
    row_block = (2, 8, 128)
    slots_x, own = call(
        pool_kernel, "pool", [fields], [(n_gx, *row_block), (2, *block)]
    )
    prepared = call(
        prepare_kernel,
        "prepare",
        [
            lift_weight,
            lift_bias[None],
            spectral_weight.reshape(2, 64, 64, 64),
            bypass_weight,
            layer_bias[None],
            mlp_in_weight,
            mlp_in_bias[None],
            mlp_out_weight.T,
            mlp_out_bias[None],
            project_weight.T,
            project_bias[None],
        ],
        [
            (PADDED * 64, 128),
            ((64, 3 * PADDED), BF16),
            ((136, 192), BF16),
            (128, 128),
            (3, 128, 128),
            (8, 128),
        ],
    )

    twins = [(i, i ^ 1) for i in range(n_gy)]
    others = [(i, (i + 1 if i % 2 else i - 1) % n_gy) for i in range(n_gy)]
    current = fields
    for step in range(STEPS):
        got_x = lax.all_to_all(slots_x, "gx", 0, 0, tiled=True)
        slots_y, strip = call(
            strip_kernel, "strip", [own, got_x, *refill, prepared[-1]], [(n_gy, *block), (3, ROWS, 128)]
        )
        got_y = lax.all_to_all(slots_y, "gy", 0, 0, tiled=True)
        twin = lax.ppermute(strip, "gy", twins)
        other = lax.ppermute(strip, "gy", others)
        operands = [
            current,
            strip,
            twin,
            other,
            got_y,
            *prepared,
            *tables,
        ]
        scratch = [pltpu.VMEM((ROWS * PADDED, 128), F32), pltpu.VMEM((ROWS * 8, 128), F32), pltpu.VMEM((3, ROWS * 8, 128), F32)]
        if step + 1 < STEPS:
            current, slots_x, own = call(
                middle_kernel,
                "middle",
                operands,
                [fields.shape, (n_gx, *row_block), (2, *block)],
                scratch,
            )
        else:
            (current,) = call(final_kernel, "final", operands, [fields.shape], scratch)
    return current


def solution(mesh):
    placed = (P(None, "gx", "gy"), P(), P(), P(), P(), P(), P(), P(), P(), P(), P(), P())
    return jax.shard_map(
        shards, mesh=mesh, in_specs=placed, out_specs=P(None, "gx", "gy"), check_vma=False
    )
```

```python
import math

import jax
import jax.numpy as jnp
import numpy as np
from jax import lax
from jax.experimental import pallas as pl
from jax.experimental.pallas import tpu as pltpu
from jax.sharding import PartitionSpec as P

STEPS = 2
ROWS = 32
COLS = 128
FEATURES = 12
PADDED = 16
LANE_L3 = 64
LANE_L2 = 80
LANE_L3_COPY = 112

BF16 = jnp.bfloat16
F32 = jnp.float32
GELU_SCALE = math.sqrt(2.0 / math.pi)


def refill_tables():
    columns = np.zeros((128, 256), np.float32)
    for cell in range(64):
        columns[cell, LANE_L2 + cell // 2] = 0.5
        columns[cell, LANE_L3 + cell // 4] = 0.25
        columns[cell, LANE_L3_COPY + cell // 4] = 0.25
    for cell in range(32):
        columns[64 + cell, 128 + LANE_L2 + cell] = 1.0
        columns[64 + cell, 128 + LANE_L3 + cell // 2] = 0.5
        columns[64 + cell, 128 + LANE_L3_COPY + cell // 2] = 0.5
    rows = np.zeros((96, 96), np.float32)
    for side in range(2):
        for channel in range(3):
            base = side * 24 + channel * 8
            for sub in range(8):
                row = (sub + 4) % 8
                if (row >= 4) == (side == 0):
                    start = base + 2 * (row % 4)
                    rows[base + sub, start : start + 2] = 0.5
                else:
                    rows[base + sub, 48 + base + sub] = 1.0
                row = (sub + 2) % 4
                if (row >= 2) == (side == 0):
                    start = base + 4 * (row % 2)
                    rows[48 + base + sub, start : start + 4] = 0.25
                else:
                    start = 48 + base + (2 * row + 4) % 8
                    rows[48 + base + sub, start : start + 2] = 0.5
    return np.concatenate([columns, columns], axis=0), np.concatenate([rows, rows], axis=1)


def pool_tables():
    cell = lax.broadcasted_iota(jnp.int32, (COLS, 128), 0)
    lane = lax.broadcasted_iota(jnp.int32, (COLS, 128), 1)
    eighth = cell >> 3
    columns = jnp.where(
        lane < LANE_L3,
        jnp.where(cell >> 1 == lane, 0.5, 0.0),
        jnp.where(
            (lane >= LANE_L2) & (lane < LANE_L3_COPY),
            jnp.where(cell >> 2 == lane - LANE_L2, 0.25, 0.0),
            jnp.where(
                (eighth == lane - LANE_L3) | (eighth == lane - LANE_L3_COPY), 0.125, 0.0
            ),
        ),
    ).astype(BF16)
    out = lax.broadcasted_iota(jnp.int32, (96, 96), 0)
    cell = lax.broadcasted_iota(jnp.int32, (96, 96), 1)
    kind = (out >> 3) & 3
    sub = out & 7
    row = cell & 31
    fine = jnp.where(row >> 1 == sub + 8 * kind, 0.5, 0.0)
    middle = jnp.where(row >> 2 == ((sub + 4) & 7), 0.25, 0.0)
    coarse = jnp.where(row >> 3 == ((sub + 2) & 3), 0.125, 0.0)
    rows = jnp.where(kind < 2, fine, jnp.where(kind == 2, middle, coarse))
    rows = jnp.where(out >> 5 == cell >> 5, rows, 0.0).astype(BF16)
    return jnp.concatenate([columns, columns], axis=0), jnp.concatenate([rows, rows], axis=1)


def fourier_tables():
    signed = np.array([0, 1, 2, 3, -4, -3, -2, -1])
    theta = 2.0 * np.pi * ((signed[:, None] * np.arange(ROWS)[None, :]) % ROWS) / ROWS
    phi = 2.0 * np.pi * ((np.arange(8)[:, None] * np.arange(COLS)[None, :]) % COLS) / COLS
    forward_rows = np.zeros((256, ROWS * PADDED))
    for feature in range(FEATURES):
        for mode in range(8):
            for row in range(ROWS):
                forward_rows[feature * 8 + mode, row * PADDED + feature] = math.cos(
                    theta[mode, row]
                )
                forward_rows[128 + feature * 8 + mode, row * PADDED + feature] = -math.sin(
                    theta[mode, row]
                )
    forward_cols = np.concatenate([np.cos(phi), -np.sin(phi)], axis=0)
    inverse_rows = np.zeros((2, 8, 8, ROWS, 2, 8))
    for mode in range(8):
        for column in range(8):
            inverse_rows[0, mode, column, :, 0, column] = np.cos(theta[mode])
            inverse_rows[1, mode, column, :, 0, column] = -np.sin(theta[mode])
            inverse_rows[0, mode, column, :, 1, column] = np.sin(theta[mode])
            inverse_rows[1, mode, column, :, 1, column] = np.cos(theta[mode])
    weight = np.where(np.arange(8) == 0, 1.0, 2.0)[:, None] / (ROWS * COLS)
    inverse_cols = np.zeros((4, 8, 16, 2, COLS))
    for pair in range(4):
        for half in range(2):
            inverse_cols[pair, 2 * pair + half, :8, half] = 0.5 * weight * np.cos(phi)
            inverse_cols[pair, 2 * pair + half, 8:, half] = -0.5 * weight * np.sin(phi)
    return (
        forward_rows,
        forward_cols,
        inverse_rows.reshape(128, 512),
        inverse_cols.reshape(4 * 128, 256),
    )


def halves_of_table(table):
    table = jnp.asarray(table.astype(np.float32))
    high = table.astype(BF16)
    low = (table - high.astype(F32)).astype(BF16)
    return high, low


def split(value):
    high = value.astype(BF16)
    return high, (value - high.astype(F32)).astype(BF16)


def matmul(left, right):
    return jnp.dot(left, right, preferred_element_type=F32)


def product(left, right):
    left_high, left_low = left
    right_high, right_low = right
    return (
        matmul(left_high, right_high) + matmul(left_high, right_low) + matmul(left_low, right_high)
    )


def gelu_of_double(half):
    inner = half * (2.0 * GELU_SCALE + (8.0 * GELU_SCALE * 0.044715) * (half * half))
    return half + half * jnp.tanh(inner)


def pooled_blocks(flat):
    pool_columns, pool_rows = pool_tables()
    high, low = split(flat)
    across = matmul(jnp.concatenate([high, low], axis=1), pool_columns)
    high, low = split(across)
    pooled = matmul(pool_rows, jnp.concatenate([high, low], axis=0))
    lane = lax.broadcasted_iota(jnp.int32, (8, 128), 1)
    first = lane < LANE_L3
    second = (lane >= LANE_L2) & (lane < LANE_L3_COPY)
    upper = []
    lower = []
    for channel in range(3):
        base = channel * 32
        coarse = jnp.where(second, pooled[base + 16 : base + 24], pooled[base + 24 : base + 32])
        upper.append(jnp.where(first, pooled[base : base + 8], coarse))
        lower.append(jnp.where(first, pooled[base + 8 : base + 16], coarse))
    return upper, lower


def emit_slots(slots_ref, position, upper, lower):
    count = slots_ref.shape[0]
    for slot in range(count):
        ahead = lax.rem(slot - position + count, count) < count // 2
        for channel in range(3):
            slots_ref[slot, channel] = jnp.where(ahead, lower[channel], upper[channel])


def near_tiles(pieces, kept):
    lane = lax.broadcasted_iota(jnp.int32, (8, 128), 1)
    shared = jnp.where(
        kept, pltpu.roll(pieces[0], 112, 1), pltpu.roll(pltpu.roll(pieces[1], 112, 1), 4, 0)
    )
    rest = jnp.where(lane < 96, shared, pltpu.roll(pieces[2], 16, 1))
    return (
        jnp.where(lane < 64, pieces[0], pltpu.roll(pieces[1], 64, 1)),
        jnp.where(lane < 64, pieces[2], rest),
    )


def far_tiles(pieces):
    lane = lax.broadcasted_iota(jnp.int32, (8, 128), 1)
    return (
        jnp.where(lane < 64, pltpu.roll(pieces[0], 64, 1), pieces[1]),
        pltpu.roll(pieces[2], 64, 1),
    )


def emit_row_slots(slots_ref, position, upper, lower):
    top = lax.broadcasted_iota(jnp.int32, (8, 128), 0) < 4
    near = near_tiles(upper, top), near_tiles(lower, jnp.logical_not(top))
    far = far_tiles(upper), far_tiles(lower)
    count = slots_ref.shape[0]
    for slot in range(count):
        distance = lax.rem(slot - position + count, count)
        ahead = distance < count // 2
        beside = (distance == 1) | (distance == count - 1)
        for tile in range(2):
            slots_ref[slot, tile] = jnp.where(
                beside,
                jnp.where(ahead, near[1][tile], near[0][tile]),
                jnp.where(ahead, far[1][tile], far[0][tile]),
            )


def received_rows(got_ref, position, columns, rows):
    lane = lax.broadcasted_iota(jnp.int32, (8, 128), 1)
    first = lane < LANE_L3
    second = (lane >= LANE_L2) & (lane < LANE_L3_COPY)
    near = {}
    for offset in (-4, -3, -2, 2, 3, 4):
        place = lax.rem(position + offset + 16, 16)
        head, tail = got_ref[place, 0], got_ref[place, 1]
        near[offset] = [pltpu.roll(head, 64, 1), head, pltpu.roll(tail, 64, 1)]
    beside = []
    for offset in (-1, 1):
        place = lax.rem(position + offset + 16, 16)
        head, tail = got_ref[place, 0], got_ref[place, 1]
        beside.append(jnp.where(first, head, tail))
        beside.append(jnp.where(first, pltpu.roll(head, 64, 1), pltpu.roll(tail, 4, 0)))
        beside.append(jnp.where(first, tail, pltpu.roll(tail, 96, 1)))
    high, low = split(jnp.concatenate(beside, axis=0))
    across = matmul(jnp.concatenate([high, low], axis=1), columns)
    high, low = split(jnp.concatenate([across[:, :128], across[:, 128:]], axis=0))
    pooled = matmul(rows, jnp.concatenate([high, low], axis=0))
    for side, offset in enumerate((-1, 1)):
        near[offset] = []
        for channel in range(3):
            base = side * 24 + channel * 8
            coarse = jnp.where(
                second, pooled[base : base + 8], pooled[48 + base : 48 + base + 8]
            )
            near[offset].append(jnp.where(first, beside[side * 3 + channel], coarse))
    return near


def pool_kernel(current_ref, slots_ref, own_ref):
    flat = current_ref[...].reshape(96, 128)
    upper, lower = pooled_blocks(flat)
    for channel in range(3):
        own_ref[0, channel] = upper[channel]
        own_ref[1, channel] = lower[channel]
    emit_row_slots(slots_ref, lax.axis_index("gx"), upper, lower)


def strip_kernel(own_ref, got_ref, columns_ref, rows_ref, ready_ref, slots_ref, strip_ref):
    received = received_rows(got_ref, lax.axis_index("gx"), columns_ref[...], rows_ref[...])
    lane = lax.broadcasted_iota(jnp.int32, (8, 128), 1)
    sub = lax.broadcasted_iota(jnp.int32, (8, 128), 0)
    first = lane < LANE_L3
    second = (lane >= LANE_L2) & (lane < LANE_L3_COPY)
    top = sub < 4
    low_two = sub < 2
    high_two = sub >= 6
    quarter = lane // 32

    upper_out = []
    lower_out = []
    for channel in range(3):
        near = {offset: blocks[channel] for offset, blocks in received.items()}
        near[0] = own_ref[0, channel]
        finest = [near[-1], own_ref[0, channel], own_ref[1, channel], near[1]]
        middle = [(-2, -1), (-1, 0), (0, 1), (1, 2)]
        coarse = [(-4, -3, -2), (-2, -1, 0), (0, 1, 2), (2, 3, 4)]
        upper = jnp.zeros((8, 128), F32)
        lower = jnp.zeros((8, 128), F32)
        for block in range(4):
            before, after = middle[block]
            start, centre, end = coarse[block]
            wide = jnp.where(
                low_two, near[start], jnp.where(high_two, near[end], near[centre])
            )
            value = jnp.where(
                first,
                finest[block],
                jnp.where(second, jnp.where(top, near[before], near[after]), wide),
            )
            strip_ref[channel, block * 8 : block * 8 + 8] = value
            here = quarter == block
            upper = jnp.where(here, pltpu.roll(value, (32 * block - 64) % 128, 1), upper)
            lower = jnp.where(here, pltpu.roll(value, (32 * block - 96) % 128, 1), lower)
        upper_out.append(upper)
        lower_out.append(lower)
    emit_slots(slots_ref, lax.axis_index("gy"), upper_out, lower_out)


def stacked_left(value):
    high, low = split(value)
    return jnp.concatenate([high, high, low], axis=1)


def stacked_right(value):
    high, low = split(value)
    return jnp.concatenate([high, low, high], axis=0)


def prepare_kernel(
    lift_ref,
    lift_bias_ref,
    weight_ref,
    bypass_ref,
    layer_bias_ref,
    mlp_in_ref,
    mlp_in_bias_ref,
    mlp_out_ref,
    mlp_out_bias_ref,
    project_ref,
    project_bias_ref,
    mixing_ref,
    skip_ref,
    inner_ref,
    inner_bias_ref,
    last_ref,
    offset_ref,
):
    highest = lax.Precision.HIGHEST
    lift = jnp.concatenate(
        [lift_ref[...], lift_bias_ref[...], jnp.zeros((PADDED - FEATURES - 1, 64), F32)], axis=0
    )
    left = stacked_left(lift)

    def mode_step(mode, carry):
        both = jnp.concatenate([weight_ref[0, mode], weight_ref[1, mode]], axis=1)
        mixing_ref[pl.ds(mode, PADDED, stride=64), :] = matmul(left, stacked_right(both))
        return carry

    lax.fori_loop(0, 64, mode_step, 0, unroll=8)

    skip = jnp.dot(lift, bypass_ref[...], precision=highest)
    row = lax.broadcasted_iota(jnp.int32, skip.shape, 0)
    skip = skip + jnp.where(row == FEATURES, layer_bias_ref[...], 0.0)
    square = jnp.concatenate([0.5 * skip, jnp.zeros((128 - PADDED, 64), F32)], axis=0)
    square = jnp.concatenate([square, jnp.zeros((128, 64), F32)], axis=1)
    skip_ref[...] = stacked_left(jnp.transpose(square)[:64, :PADDED])

    project = jnp.concatenate([project_ref[...], jnp.zeros((5, 64), F32)], axis=0)
    wide = jnp.concatenate([mlp_in_ref[...], jnp.zeros((64, 128), F32)], axis=0)
    inner = jnp.concatenate([0.5 * jnp.transpose(wide)[:, :64], project], axis=0)
    inner_ref[...] = stacked_left(inner)
    inner_bias_ref[...] = jnp.transpose(
        jnp.broadcast_to(0.5 * mlp_in_bias_ref[...], (128, 128))
    )
    last = jnp.dot(project, mlp_out_ref[...], precision=highest)
    for channel in range(3):
        last_ref[channel] = jnp.transpose(
            jnp.broadcast_to(last[channel : channel + 1], (128, 128))
        )
    sub = lax.broadcasted_iota(jnp.int32, (8, 3), 0)
    lane = lax.broadcasted_iota(jnp.int32, (8, 3), 1)
    constant = jnp.sum(project * mlp_out_bias_ref[...], axis=1, keepdims=True) + jnp.sum(
        jnp.where(sub == lane, project_bias_ref[...], 0.0), axis=1, keepdims=True
    )
    offset_ref[...] = jnp.broadcast_to(constant, (8, 128))


def contexts(strip_ref, twin_ref, other_ref, got_ref, position, channel, block):
    lane = lax.broadcasted_iota(jnp.int32, (8, 128), 1)
    rows = slice(block * 8, block * 8 + 8)
    here = strip_ref[channel, rows]
    twin = twin_ref[channel, rows]
    other = other_ref[channel, rows]
    even = position % 2 == 0
    before = jnp.where(even, other, twin)
    after = jnp.where(even, twin, other)
    far = {
        offset: got_ref[lax.rem(position + offset + 32, 32), channel]
        for offset in (-4, -3, -2, 2, 3, 4)
    }
    packed = 32 * block

    def moved(value, source, target):
        shift = (target - source) % 128
        return value if shift == 0 else pltpu.roll(value, shift, 1)

    def gathered(pieces):
        result = moved(*pieces[-1][1:])
        for piece in reversed(pieces[:-1]):
            result = jnp.where(lane < piece[0], moved(*piece[1:]), result)
        return result

    first = gathered([(32, before, 32, 0), (96, here, 0, 32), (128, after, 0, 96)])
    second = gathered(
        [
            (16, far[-2], packed, 0),
            (48, before, LANE_L2, 16),
            (80, here, LANE_L2, 48),
            (112, after, LANE_L2, 80),
            (128, far[2], packed + 16, 112),
        ]
    )
    third = gathered(
        [
            (8, far[-4], packed + 24, 0),
            (24, far[-3], packed + 16, 8),
            (40, far[-2], packed + 16, 24),
            (56, before, LANE_L3, 40),
            (72, here, LANE_L3, 56),
            (88, after, LANE_L3, 72),
            (104, far[2], packed, 88),
            (120, far[3], packed, 104),
            (128, far[4], packed, 120),
        ]
    )
    return first, second, third


def tile_step(
    current_ref,
    strip_ref,
    twin_ref,
    other_ref,
    got_ref,
    mixing_ref,
    skip_ref,
    inner_ref,
    inner_bias_ref,
    last_ref,
    offset_ref,
    rows_high_ref,
    rows_low_ref,
    cols_high_ref,
    cols_low_ref,
    back_rows_high_ref,
    back_rows_low_ref,
    back_cols_high_ref,
    back_cols_low_ref,
    features_ref,
    results_ref,
    partial_ref,
):
    position = lax.axis_index("gy")
    for channel in range(3):
        for block in range(4):
            pieces = (
                current_ref[channel, block * 8 : block * 8 + 8],
                *contexts(strip_ref, twin_ref, other_ref, got_ref, position, channel, block),
            )
            for level in range(4):
                features_ref[
                    pl.ds(block * 8 * PADDED + level * 3 + channel, 8, stride=PADDED), :
                ] = pieces[level]
    for row in range(ROWS):
        tail = lax.broadcasted_iota(jnp.int32, (4, 128), 0)
        features_ref[row * PADDED + FEATURES : (row + 1) * PADDED, :] = jnp.where(
            tail == 0, 1.0, 0.0
        )

    features = split(features_ref[...])
    along_rows = product((rows_high_ref[...], rows_low_ref[...]), features)
    contract = (((1,), (1,)), ((), ()))
    along_high, along_low = split(along_rows)

    def transposed(left, right):
        return lax.dot_general(left, right, contract, preferred_element_type=F32)

    spectrum = (
        transposed(cols_high_ref[...], along_high)
        + transposed(cols_high_ref[...], along_low)
        + transposed(cols_low_ref[...], along_high)
    )
    real = spectrum[:8, :128] - spectrum[8:, 128:]
    imag = spectrum[8:, :128] + spectrum[:8, 128:]
    lane = lax.broadcasted_iota(jnp.int32, (8, 128), 1)
    sub = lax.broadcasted_iota(jnp.int32, (8, 128), 0)
    real = jnp.where(
        (lane == 8 * FEATURES) & (sub == 0), float(ROWS * COLS), jnp.where(lane < 96, real, 0.0)
    )
    modes = []
    sign = jnp.where(lane < 64, -1.0, 1.0)
    for mode in range(8):
        with_real = None
        with_imag = None
        for feature in range(FEATURES + (1 if mode == 0 else 0)):
            place = feature * 8 + mode
            weights = mixing_ref[feature * 64 + mode * 8 : feature * 64 + mode * 8 + 8, :]
            term = jnp.broadcast_to(real[:, place : place + 1], (8, 128)) * weights
            with_real = term if with_real is None else with_real + term
            if feature < FEATURES:
                term = jnp.broadcast_to(imag[:, place : place + 1], (8, 128)) * weights
                with_imag = term if with_imag is None else with_imag + term
        modes.append(with_real + sign * pltpu.roll(with_imag, 64, 1))
    turned = jnp.transpose(jnp.concatenate(modes, axis=0))
    outputs = split(jnp.concatenate([turned[:64], turned[64:]], axis=1))
    back = product(outputs, (back_rows_high_ref[...], back_rows_low_ref[...]))
    stacked = split(
        jnp.concatenate([back[:, 128 * block : 128 * block + 128] for block in range(4)], axis=0)
    )

    skip = skip_ref[...]
    inner_left = inner_ref[...]
    inner_bias = jnp.concatenate([inner_bias_ref[...], inner_bias_ref[...]], axis=1)
    offset = jnp.concatenate([offset_ref[...], offset_ref[...]], axis=1)
    pending = []

    def finish(row, mixed):
        wide = matmul(inner_left, stacked_right(mixed))
        hidden = gelu_of_double(wide[:128] + inner_bias)
        total = wide[128:136] + offset
        for half in range(2):
            lanes = slice(half * 128, half * 128 + 128)
            results_ref[(row + half) * 8 : (row + half) * 8 + 8, :] = total[:, lanes]
            for channel in range(3):
                partial_ref[channel, (row + half) * 8 : (row + half) * 8 + 8] = jnp.sum(
                    (hidden[:, lanes] * last_ref[channel]).reshape(16, 8, 128), axis=0
                )

    for pair in range(4):
        table = (
            back_cols_high_ref[pair * 128 : pair * 128 + 128, :],
            back_cols_low_ref[pair * 128 : pair * 128 + 128, :],
        )
        spectral = matmul(
            jnp.concatenate([stacked[0], stacked[0], stacked[1]], axis=1),
            jnp.concatenate([table[0], table[1], table[0]], axis=0),
        )
        for block in range(4):
            row = block * 8 + pair * 2
            high, low = (
                jnp.concatenate(
                    [
                        half[row * PADDED : (row + 1) * PADDED],
                        half[(row + 1) * PADDED : (row + 2) * PADDED],
                    ],
                    axis=1,
                )
                for half in features
            )
            cells = jnp.concatenate([high, low, high], axis=0)
            pending.append(
                (
                    row,
                    gelu_of_double(
                        spectral[block * 64 : block * 64 + 64] + matmul(skip, cells)
                    ),
                )
            )
            if len(pending) == 2:
                finish(*pending.pop(0))
    finish(*pending.pop(0))

    def sublane_sum(channel):
        total = results_ref[pl.ds(channel, ROWS, stride=8), :]
        for sub in range(8):
            total = total + partial_ref[channel, pl.ds(sub, ROWS, stride=8), :]
        return total

    return [current_ref[channel] + sublane_sum(channel) for channel in range(3)]


def final_kernel(*refs):
    next_ref = refs[19]
    updated = tile_step(*refs[:19], *refs[20:])
    for channel in range(3):
        next_ref[channel] = updated[channel]


def middle_kernel(*refs):
    next_ref, slots_ref, own_ref = refs[19:22]
    updated = tile_step(*refs[:19], *refs[22:])
    for channel in range(3):
        next_ref[channel] = updated[channel]
    upper, lower = pooled_blocks(jnp.concatenate(updated, axis=0))
    for channel in range(3):
        own_ref[0, channel] = upper[channel]
        own_ref[1, channel] = lower[channel]
    emit_row_slots(slots_ref, lax.axis_index("gx"), upper, lower)


VMEM = pl.BlockSpec(memory_space=pltpu.VMEM)


def resident(operand):
    return pltpu.with_memory_space_constraint(operand, pltpu.VMEM)


def call(body, name, operands, results, scratch=(), resident_out=True):
    return pl.pallas_call(
        body,
        name=name,
        out_shape=[
            (pltpu.VMEM if resident_out else jax.ShapeDtypeStruct)(
                *(r if isinstance(r[0], tuple) else (r, F32))
            )
            for r in results
        ],
        in_specs=[VMEM] * len(operands),
        out_specs=[VMEM] * len(results),
        scratch_shapes=list(scratch),
        compiler_params=pltpu.CompilerParams(vmem_limit_bytes=16 << 20),
    )(
        *(
            operand if operand.ndim == 4 and operand.shape[1] == 64 else resident(operand)
            for operand in operands
        )
    )


def shards(
    fields,
    lift_weight,
    lift_bias,
    spectral_weight,
    bypass_weight,
    layer_bias,
    mlp_in_weight,
    mlp_in_bias,
    mlp_out_weight,
    mlp_out_bias,
    project_weight,
    project_bias,
):
    n_gx = lax.axis_size("gx")
    n_gy = lax.axis_size("gy")
    tables = [half for table in fourier_tables() for half in halves_of_table(table)]

    refill = [jnp.asarray(table).astype(BF16) for table in refill_tables()]

    block = (3, 8, 128)
    row_block = (2, 8, 128)
    slots_x, own = call(
        pool_kernel, "pool", [fields], [(n_gx, *row_block), (2, *block)]
    )
    prepared = call(
        prepare_kernel,
        "prepare",
        [
            lift_weight,
            lift_bias[None],
            spectral_weight.reshape(2, 64, 64, 64),
            bypass_weight,
            layer_bias[None],
            mlp_in_weight,
            mlp_in_bias[None],
            mlp_out_weight.T,
            mlp_out_bias[None],
            project_weight.T,
            project_bias[None],
        ],
        [
            (PADDED * 64, 128),
            ((64, 3 * PADDED), BF16),
            ((136, 192), BF16),
            (128, 128),
            (3, 128, 128),
            (8, 128),
        ],
    )

    twins = [(i, i ^ 1) for i in range(n_gy)]
    others = [(i, (i + 1 if i % 2 else i - 1) % n_gy) for i in range(n_gy)]
    current = fields
    for step in range(STEPS):
        got_x = lax.all_to_all(slots_x, "gx", 0, 0, tiled=True)
        slots_y, strip = call(
            strip_kernel, "strip", [own, got_x, *refill, prepared[-1]], [(n_gy, *block), (3, ROWS, 128)]
        )
        got_y = lax.all_to_all(slots_y, "gy", 0, 0, tiled=True)
        twin = lax.ppermute(strip, "gy", twins)
        other = lax.ppermute(strip, "gy", others)
        operands = [
            current,
            strip,
            twin,
            other,
            got_y,
            *prepared,
            *tables,
        ]
        scratch = [pltpu.VMEM((ROWS * PADDED, 128), F32), pltpu.VMEM((ROWS * 8, 128), F32), pltpu.VMEM((3, ROWS * 8, 128), F32)]
        if step + 1 < STEPS:
            current, slots_x, own = call(
                middle_kernel,
                "middle",
                operands,
                [fields.shape, (n_gx, *row_block), (2, *block)],
                scratch,
            )
        else:
            (current,) = call(
                final_kernel, "final", operands, [fields.shape], scratch, resident_out=False
            )
    return current


def solution(mesh):
    placed = (P(None, "gx", "gy"), P(), P(), P(), P(), P(), P(), P(), P(), P(), P(), P())
    return jax.shard_map(
        shards, mesh=mesh, in_specs=placed, out_specs=P(None, "gx", "gy"), check_vma=False
    )
```
